512 devices in a mesh: year: 32 (over x_hi, y, core), port: 16 (over z, x_lo).
Axes of the slice: x: 4 (x_hi: 2, x_lo: 2; x = x_hi * 2 + x_lo), y: 8, z: 8, core: 2. Of those that a mesh axis runs over, the one named last changes fastest.
Arguments:
- event_loss: bfloat16 [16384, 16384], P('year', 'port'), may hold values from 0 to 24
- event_year: int32 [16384], P('year'), may hold values from -1 to 1023, as said below
- retention: float32 [16384], P('port'), may hold values from 0.2 to 2
- risk_limit: float32 [16384], P('port'), may hold values from 1 to 8
- cession_share: bfloat16 [16384, 4], P('port'), may hold values from 0.099609375 to 1
- member_treaty: int32 [16384, 4], P('port'), may hold values from 0 to 1023, all different within a row
- attach_tier: int32 [1024], P('port'), may hold values from 2 to 11
- limit_tier: int32 [1024], P('port'), may hold values from 2 to 10
- reinstatements: int32 [1024], P('port'), may hold values from 0 to 3
- reinstate_rate: float32 [1024], P('port'), may hold values from 0.1 to 1
- stop_attach: float32 [1024], P('port'), may hold values from 0.7 to 2
- stop_width: float32 [1024], P('port'), may hold values from 0.3 to 2
Outputs:
- layer_net: float32 [1024, 1024], P('port', 'year')
- stop_loss: float32 [1024, 1024], P('port', 'year')
- tail_mean: float32 [1024], P('port')
The draws below stay inside these ranges and needn't reach their ends.
Inputs may be any that keep to these rules, and one draw needn't show every extreme that they name: `event_year`: the 512 rows of year-block b name years b * 32 to (b + 1) * 32 - 1 in nondecreasing order, followed by padding rows marked -1; at least one block has no padding row. `member_treaty`: each portfolio names 4 different treaties, and every treaty is named by some portfolio.
All inputs are finite; a program needn't handle non-finite values.
Results may differ from the reference program's by a relative error of at most 0.029.
Values may be sent and summed in bfloat16 or wider, within the bound.
No kernel may reach another device: no remote copies, remote signals or barrier semaphores. Data moves between devices by JAX's collectives and lax.ppermute only.
A program may use at most 64 MiB of HBM per device.

```python
import math
import jax
import jax.numpy as jnp
from jax import lax

PORT_DEV = 1024
TREATIES = 1024
MEMB = 4
YEAR_DEV = 32
TAIL = 16
ROWS_DEV = 512
PORTS = 16384
YEARS = 1024
EVENT_ROWS = 16384
N_YEAR = 32
N_PORT = 16


def draw_event_loss(key, part):
    key_row, key_col, key_cell = jax.random.split(key, 3)
    position = jnp.arange(EVENT_ROWS, dtype=jnp.float32) / EVENT_ROWS
    rising = jnp.exp(math.log(3.0) * position)
    col_scale = jnp.exp(jax.random.uniform(key_col, (PORTS,), jnp.float32, math.log(0.3), math.log(3.0)))
    row_scale = jnp.exp(jax.random.uniform(key_row, (EVENT_ROWS,), jnp.float32, math.log(0.5), math.log(2.0)))
    cell = jnp.exp(jax.random.uniform(key_cell, (EVENT_ROWS, PORTS), jnp.float32, math.log(0.2), math.log(5.0)))
    value = 0.2 * (rising * row_scale)[:, None] * col_scale[None, :] * cell
    return value.astype(jnp.bfloat16)


def draw_event_year(key, part):
    key_fill, key_full, key_year = jax.random.split(key, 3)
    block_total = EVENT_ROWS // ROWS_DEV
    halvings = jax.random.randint(key_fill, (block_total,), 0, 4).astype(jnp.int32)
    live_rows = jnp.right_shift(jnp.full((block_total,), ROWS_DEV, jnp.int32), halvings)
    full_block = jax.random.randint(key_full, (), 0, block_total).astype(jnp.int32)
    block_index = jnp.arange(block_total, dtype=jnp.int32)
    live_rows = jnp.where(block_index == full_block, ROWS_DEV, live_rows)
    years = jax.random.randint(key_year, (block_total, ROWS_DEV), 0, YEAR_DEV).astype(jnp.int32)
    slot_index = jnp.arange(ROWS_DEV, dtype=jnp.int32)
    years = jnp.where(slot_index[None, :] < live_rows[:, None], years, YEAR_DEV)
    years = jnp.sort(years, axis=1)
    marked = jnp.where(years < YEAR_DEV, years + block_index[:, None] * YEAR_DEV, -1)
    return marked.reshape(EVENT_ROWS).astype(jnp.int32)


def set_ends(entries, rng, smallest, high):
    place = [jax.random.randint(jax.random.fold_in(rng, axis), (), 0, length) for axis, length in enumerate(entries.shape)]
    main_axis = entries.shape.index(max(entries.shape))
    next_to = place[:main_axis] + [(place[main_axis] + 1) % entries.shape[main_axis]] + place[main_axis + 1:]
    return entries.at[tuple(place)].set(smallest).at[tuple(next_to)].set(high)


def block_levels(key, dims, pieces, smallest, top_value):
    def one(dim, parts):
        draws = jax.random.uniform(jax.random.fold_in(jax.random.fold_in(key, 6), dim), (parts,), jnp.float32, smallest / len(pieces), top_value / len(pieces))
        return jnp.repeat(jnp.exp(draws), dims[dim] // parts).reshape((-1,) + (1,) * (len(dims) - dim - 1))

    level = one(*pieces[0])
    for cut in pieces[1:]:
        level = level * one(*cut)
    return level


def distinct(stream_key, rows, count, top, lift):
    sequence = jax.random.permutation(jax.random.fold_in(stream_key, 1), count)
    boost = sequence
    for power in range(3):
        boost = boost * boost // count
    boost = boost * lift // count
    lots = jax.random.randint(jax.random.fold_in(stream_key, 2), (rows, count), 0, 4096) + boost
    sure = jax.random.permutation(jax.random.fold_in(stream_key, 3), rows)[jnp.arange(count) % rows]
    lots = jnp.where(jnp.arange(rows)[:, None] == sure[None, :], 1 << 14, lots)
    merit = lots * count + jnp.arange(count)
    return lax.top_k(merit.astype(jnp.int32), top)[1].astype(jnp.int32)


def setup_inputs(seed: int = 0) -> dict:
    streams_of = jax.random.split(jax.random.key(seed), 13)
    return {
        "event_loss": draw_event_loss(jax.random.fold_in(streams_of[12], 71), 0),
        "event_year": draw_event_year(jax.random.fold_in(streams_of[12], 71), 0),
        "retention": jnp.clip(jnp.exp(math.log(2.0) - 2.3025851 * jax.random.uniform(streams_of[2], (PORTS,), jnp.float32) ** block_levels(streams_of[2], (PORTS,), ((0, 16),), -0.2, 0.2)), 0.2, 2.0),
        "risk_limit": jnp.clip(jnp.exp(math.log(8.0) - 2.0794415 * jax.random.uniform(streams_of[3], (PORTS,), jnp.float32) ** block_levels(streams_of[3], (PORTS,), ((0, 16),), -0.2, 0.2)), 1.0, 8.0),
        "cession_share": jnp.clip(jnp.exp(math.log(1.0) - 2.306499 * jax.random.uniform(streams_of[4], (PORTS, MEMB), jnp.float32) ** block_levels(streams_of[4], (PORTS, MEMB), ((0, 16),), -0.2, 0.2)), 0.099609375, 1.0).astype(jnp.bfloat16),
        "member_treaty": distinct(streams_of[5], PORTS, TREATIES, MEMB, 32),
        "attach_tier": set_ends(jax.random.randint(streams_of[6], (TREATIES,), 2, 12), jax.random.fold_in(streams_of[6], 1), 2, 11).astype(jnp.int32),
        "limit_tier": set_ends(jax.random.randint(streams_of[7], (TREATIES,), 2, 11), jax.random.fold_in(streams_of[7], 1), 2, 10).astype(jnp.int32),
        "reinstatements": set_ends(jax.random.randint(streams_of[8], (TREATIES,), 0, 4), jax.random.fold_in(streams_of[8], 1), 0, 3).astype(jnp.int32),
        "reinstate_rate": jnp.clip(jnp.exp(math.log(1.0) - 2.3025851 * jax.random.uniform(streams_of[9], (TREATIES,), jnp.float32) ** block_levels(streams_of[9], (TREATIES,), ((0, 16),), -0.2, 0.2)), 0.1, 1.0),
        "stop_attach": jnp.clip(jnp.exp(math.log(2.0) - 1.0498221 * jax.random.uniform(streams_of[10], (TREATIES,), jnp.float32) ** block_levels(streams_of[10], (TREATIES,), ((0, 16),), -0.2, 0.2)), 0.7, 2.0),
        "stop_width": jnp.clip(jnp.exp(math.log(2.0) - 1.89712 * jax.random.uniform(streams_of[11], (TREATIES,), jnp.float32) ** block_levels(streams_of[11], (TREATIES,), ((0, 16),), -0.2, 0.2)), 0.3, 2.0),
    }


UNIT_LOSS = 1.0


def clamp_between(values, lower, upper):
    return jnp.minimum(jnp.maximum(values, lower), upper)


def block_tables(loss_block, year_block, first_year, retention, risk_limit, cession_share, member_treaty, attach_tier, limit_tier):
    ceded_loss = clamp_between(loss_block.astype(jnp.float32) - retention[None, :], 0.0, risk_limit[None, :]).astype(jnp.bfloat16)
    ceded_cols = lax.optimization_barrier(ceded_loss).astype(jnp.float32).T
    shard_ids = (jnp.arange(PORT_DEV * N_PORT, dtype=jnp.int32) // PORT_DEV) * TREATIES
    shard_sums = jnp.zeros((N_PORT * TREATIES, ceded_cols.shape[1]), jnp.float32)
    for member_slot in range(MEMB):
        weight_col = cession_share[:, member_slot].astype(jnp.float32)
        segment_ids = (shard_ids + member_treaty[:, member_slot]).astype(jnp.int32)
        shard_sums = shard_sums + jax.ops.segment_sum(ceded_cols * weight_col[:, None], segment_ids, N_PORT * TREATIES)
    rounded = lax.optimization_barrier(shard_sums.astype(jnp.bfloat16)).astype(jnp.float32)
    event_treaty = jnp.sum(rounded.reshape(N_PORT, TREATIES, ceded_cols.shape[1]), axis=0)
    attach = attach_tier.astype(jnp.float32) * UNIT_LOSS
    limit_loss = limit_tier.astype(jnp.float32) * UNIT_LOSS
    recovered = clamp_between(event_treaty - attach[:, None], 0.0, limit_loss[:, None])
    retained = event_treaty - recovered
    local_year = (year_block - first_year).astype(jnp.int32)
    year_hits = (local_year[:, None] == jnp.arange(YEAR_DEV, dtype=jnp.int32)[None, :]).astype(jnp.float32)
    annual = jnp.dot(recovered, year_hits, precision=lax.Precision.HIGHEST, preferred_element_type=jnp.float32)
    kept_annual = jnp.dot(retained, year_hits, precision=lax.Precision.HIGHEST, preferred_element_type=jnp.float32)
    return annual, kept_annual


def reference(event_loss, event_year, retention, risk_limit, cession_share, member_treaty, attach_tier, limit_tier, reinstatements, reinstate_rate, stop_attach, stop_width):
    loss_blocks = event_loss.reshape(N_YEAR, ROWS_DEV, PORTS)
    year_blocks = event_year.reshape(N_YEAR, ROWS_DEV)
    first_years = jnp.arange(N_YEAR, dtype=jnp.int32) * YEAR_DEV

    def one_block(inputs):
        return block_tables(inputs[0], inputs[1], inputs[2], retention, risk_limit, cession_share, member_treaty, attach_tier, limit_tier)

    annual, kept_annual = lax.map(one_block, (loss_blocks, year_blocks, first_years))
    annual = jnp.transpose(annual, (1, 0, 2)).reshape(TREATIES, YEARS)
    kept_annual = jnp.transpose(kept_annual, (1, 0, 2)).reshape(TREATIES, YEARS)
    limit_loss = limit_tier.astype(jnp.float32) * UNIT_LOSS
    reinstated = reinstatements.astype(jnp.float32)
    layer_paid = jnp.minimum(annual, ((1.0 + reinstated) * limit_loss)[:, None])
    layer_net = (layer_paid - reinstate_rate[:, None] * jnp.minimum(layer_paid, (reinstated * limit_loss)[:, None])) / limit_loss[:, None]
    base_loss = UNIT_LOSS + jnp.sum(kept_annual, axis=1) / YEARS
    loss_ratio = kept_annual / base_loss[:, None]
    stop_loss = clamp_between(loss_ratio - stop_attach[:, None], 0.0, stop_width[:, None])
    tail_mean = jnp.mean(jnp.sort(loss_ratio, axis=1)[:, YEARS - TAIL:], axis=1)
    return layer_net, stop_loss, tail_mean
```

```python
import jax
import jax.numpy as jnp
from jax import lax
from jax.experimental import pallas as pl
from jax.experimental.pallas import tpu as pltpu
from jax.sharding import PartitionSpec as P

TREATIES = 1024
MEMB = 4
YEAR_DEV = 32
TAIL = 16
LANES = 128
BLOCK = 256

UNIT_LOSS = 1.0

VMEM = pl.BlockSpec(memory_space=pltpu.VMEM)
ANY = pl.BlockSpec(memory_space=pl.ANY)
PARAMS = pltpu.CompilerParams(vmem_limit_bytes=16 * 1024 * 1024)
BY_ROWS = (((1,), (1,)), ((), ()))


def clamp_between(values, lower, upper):
    return jnp.minimum(jnp.maximum(values, lower), upper)


def shard_sums_kernel(
    loss_hbm, retention, risk_limit, share, member, sums, loss, weights, ceded, arrived
):
    fetch = pltpu.make_async_copy(loss_hbm, loss, arrived)
    fetch.start()
    columns = loss.shape[1]
    treaty = lax.broadcasted_iota(jnp.int32, (BLOCK, LANES), 0)
    treaty = treaty.astype(jnp.float32).astype(jnp.bfloat16)
    zero = jnp.zeros((BLOCK, LANES), jnp.bfloat16)
    named = member[...]
    part = share[...]
    for first in range(0, TREATIES, BLOCK):
        local = named - first
        inside = (local >= 0) & (local < BLOCK)
        local = jnp.where(inside, local, BLOCK).astype(jnp.float32).astype(jnp.bfloat16)
        for at in range(0, columns, LANES):
            block = zero
            for slot in range(MEMB):
                hit = treaty == local[slot : slot + 1, at : at + LANES]
                block = jnp.where(hit, part[slot : slot + 1, at : at + LANES], block)
            weights[first : first + BLOCK, at : at + LANES] = block
    fetch.wait()
    ceded[...] = clamp_between(
        loss[...].astype(jnp.float32) - retention[...], 0.0, risk_limit[...]
    ).astype(jnp.bfloat16)
    for first in range(0, TREATIES, BLOCK):
        sums[first : first + BLOCK, :] = lax.dot_general(
            weights[first : first + BLOCK, :],
            ceded[...],
            BY_ROWS,
            preferred_element_type=jnp.float32,
        ).astype(jnp.bfloat16)


def shard_sums(event_loss, retention, risk_limit, cession_share, member_treaty):
    rows, columns = event_loss.shape
    return pl.pallas_call(
        shard_sums_kernel,
        out_shape=jax.ShapeDtypeStruct((TREATIES, rows), jnp.bfloat16),
        in_specs=[ANY, VMEM, VMEM, VMEM, VMEM],
        out_specs=VMEM,
        scratch_shapes=[
            pltpu.VMEM((rows, columns), jnp.bfloat16),
            pltpu.VMEM((TREATIES, columns), jnp.bfloat16),
            pltpu.VMEM((rows, columns), jnp.bfloat16),
            pltpu.SemaphoreType.DMA,
        ],
        compiler_params=PARAMS,
        name="shard_sums",
    )(
        event_loss,
        retention.reshape(1, -1),
        risk_limit.reshape(1, -1),
        cession_share.T,
        member_treaty.T,
    )


def as_column(row):
    count = row.shape[1]
    down = lax.broadcasted_iota(jnp.int32, (count, count), 0)
    across = lax.broadcasted_iota(jnp.int32, (count, count), 1)
    return jnp.sum(jnp.where(down == across, row, 0.0), axis=1, keepdims=True)


def in_two(values):
    high = values.astype(jnp.bfloat16)
    low = (values - high.astype(jnp.float32)).astype(jnp.bfloat16)
    return [high, low]


def annual_kernel(
    blocks, event_year, attach_tier, limit_tier, reinstatements, reinstate_rate, net, kept, sent
):
    count = attach_tier.shape[1]
    total = blocks[0].astype(jnp.float32)
    for shard in range(1, blocks.shape[0]):
        total = total + blocks[shard].astype(jnp.float32)
    attach = attach_tier[...].astype(jnp.float32) * UNIT_LOSS
    limit = limit_tier[...].astype(jnp.float32) * UNIT_LOSS
    recovered = clamp_between(total - as_column(attach), 0.0, as_column(limit))
    retained = total - recovered
    year = event_year[...]
    local_year = jnp.where(year < 0, -1, year & (YEAR_DEV - 1))
    hits = lax.broadcasted_iota(jnp.int32, (YEAR_DEV, year.shape[1]), 0) == local_year
    hits = jnp.where(hits, 1.0, 0.0).astype(jnp.bfloat16)
    pieces = jnp.concatenate(in_two(recovered) + in_two(retained), axis=0)
    yearly = lax.dot_general(hits, pieces, BY_ROWS, preferred_element_type=jnp.float32)
    annual = yearly[:, :count] + yearly[:, count : 2 * count]
    kept_annual = yearly[:, 2 * count : 3 * count] + yearly[:, 3 * count :]
    again = reinstatements[...].astype(jnp.float32)
    paid = jnp.minimum(annual, (1.0 + again) * limit)
    net[...] = (paid - reinstate_rate[...] * jnp.minimum(paid, again * limit)) / limit
    kept[...] = kept_annual
    half = YEAR_DEV // 2
    line = jnp.concatenate((kept_annual[:half], kept_annual[half:]), axis=1)
    for peer in range(sent.shape[0]):
        sent[peer] = line


def annual_tables(
    blocks, event_year, attach_tier, limit_tier, reinstatements, reinstate_rate, peers
):
    count = attach_tier.shape[0]
    table = jax.ShapeDtypeStruct((YEAR_DEV, count), jnp.float32)
    return pl.pallas_call(
        annual_kernel,
        out_shape=(
            table,
            table,
            jax.ShapeDtypeStruct((peers, YEAR_DEV // 2, 2 * count), jnp.float32),
        ),
        in_specs=[VMEM] * 6,
        out_specs=(VMEM, VMEM, VMEM),
        compiler_params=PARAMS,
        name="annual_tables",
    )(
        blocks,
        event_year.reshape(1, -1),
        attach_tier.reshape(1, -1),
        limit_tier.reshape(1, -1),
        reinstatements.reshape(1, -1),
        reinstate_rate.reshape(1, -1),
    )


def exchange(items, low, high):
    items[low], items[high] = (
        jnp.maximum(items[low], items[high]),
        jnp.minimum(items[low], items[high]),
    )


def sort_falling(items):
    count = len(items)
    step = 1
    while step < count:
        gap = step
        while gap >= 1:
            for base in range(gap % step, count - gap, 2 * gap):
                for at in range(base, base + min(gap, count - base - gap)):
                    if at // (2 * step) == (at + gap) // (2 * step):
                        exchange(items, at, at + gap)
            gap //= 2
        step *= 2


def larger_half(first, second):
    return [jnp.maximum(one, two) for one, two in zip(first, reversed(second))]


def sort_bitonic(items):
    gap = len(items) // 2
    while gap >= 1:
        for at in range(len(items)):
            if at & gap == 0:
                exchange(items, at, at + gap)
        gap //= 2


def outcome_kernel(everyone, kept, stop_attach, stop_width, stop_loss, tail_mean):
    peers, rows, lanes = everyone.shape
    count = lanes // 2
    tiles = [
        everyone[peer, at : at + 8, :] for peer in range(peers) for at in range(0, rows, 8)
    ]
    total = tiles[0]
    for tile in tiles[1:]:
        total = total + tile
    summed = jnp.sum(total, axis=0, keepdims=True)
    summed = summed + pltpu.roll(summed, count, 1)
    base_loss = UNIT_LOSS + summed / (peers * YEAR_DEV)
    largest = None
    for at in range(0, len(tiles), TAIL):
        group = tiles[at : at + TAIL]
        sort_falling(group)
        if largest is None:
            largest = group
        else:
            largest = larger_half(largest, group)
            sort_bitonic(largest)
    for shift in (4, 2, 1):
        largest = larger_half(largest, [pltpu.roll(item, shift, 0) for item in largest])
        sort_bitonic(largest)
    largest = larger_half(largest, [pltpu.roll(item, count, 1) for item in largest])
    top = largest[0]
    for item in largest[1:]:
        top = top + item
    tail_mean[...] = (top[0:1, :] / base_loss / TAIL)[:, :count]
    stop_loss[...] = clamp_between(
        kept[...] / base_loss[:, :count] - stop_attach[...], 0.0, stop_width[...]
    )


def outcomes(everyone, kept, stop_attach, stop_width):
    count = stop_attach.shape[0]
    return pl.pallas_call(
        outcome_kernel,
        out_shape=(
            jax.ShapeDtypeStruct(kept.shape, jnp.float32),
            jax.ShapeDtypeStruct((1, count), jnp.float32),
        ),
        in_specs=[VMEM] * 4,
        out_specs=(VMEM, VMEM),
        compiler_params=PARAMS,
        name="outcomes",
    )(everyone, kept, stop_attach.reshape(1, -1), stop_width.reshape(1, -1))


def on_device(
    event_loss,
    event_year,
    retention,
    risk_limit,
    cession_share,
    member_treaty,
    attach_tier,
    limit_tier,
    reinstatements,
    reinstate_rate,
    stop_attach,
    stop_width,
):
    ports = lax.axis_size("port")
    sums = shard_sums(event_loss, retention, risk_limit, cession_share, member_treaty)
    blocks = lax.all_to_all(
        sums.reshape(ports, -1, sums.shape[1]), "port", 0, 0, tiled=True
    )
    net, kept, sent = annual_tables(
        blocks,
        event_year,
        attach_tier,
        limit_tier,
        reinstatements,
        reinstate_rate,
        lax.axis_size("year"),
    )
    everyone = lax.all_to_all(sent, "year", 0, 0, tiled=True)
    stop_loss, tail_mean = outcomes(everyone, kept, stop_attach, stop_width)
    return (net.T, stop_loss.T, tail_mean.reshape(-1))


def solution(mesh):
    return jax.shard_map(
        on_device,
        mesh=mesh,
        in_specs=(
            P("year", "port"),
            P("year"),
            P("port"),
            P("port"),
            P("port", None),
            P("port", None),
            P("port"),
            P("port"),
            P("port"),
            P("port"),
            P("port"),
            P("port"),
        ),
        out_specs=(P("port", "year"), P("port", "year"), P("port")),
        check_vma=False,
    )
```

```python
import jax
import jax.numpy as jnp
from jax import lax
from jax.experimental import pallas as pl
from jax.experimental.pallas import tpu as pltpu
from jax.sharding import PartitionSpec as P

TREATIES = 1024
MEMB = 4
YEAR_DEV = 32
TAIL = 16
LANES = 128
BLOCK = 256

UNIT_LOSS = 1.0

VMEM = pl.BlockSpec(memory_space=pltpu.VMEM)
HBM = pl.BlockSpec(memory_space=pltpu.HBM)
PARAMS = pltpu.CompilerParams(vmem_limit_bytes=16 * 1024 * 1024)
BY_ROWS = (((1,), (1,)), ((), ()))


def clamp_between(values, lower, upper):
    return jnp.minimum(jnp.maximum(values, lower), upper)


def shard_sums_kernel(*refs):
    inputs, (sums, table, hits), held = refs[:12], refs[12:15], refs[15:27]
    weights, ceded, arrived = refs[27:]
    order = (5, 4, 2, 3, 0, 1, 6, 7, 8, 9, 10, 11)
    fetches = {
        k: pltpu.make_async_copy(inputs[k], held[k], arrived.at[k]) for k in order
    }
    for k in order:
        fetches[k].start()
    loss, year, retention, risk_limit, share, member = held[:6]
    columns = loss.shape[1]
    treaty = lax.broadcasted_iota(jnp.int32, (BLOCK, LANES), 0)
    treaty = treaty.astype(jnp.float32).astype(jnp.bfloat16)
    zero = jnp.zeros((BLOCK, LANES), jnp.bfloat16)
    fetches[5].wait()
    fetches[4].wait()
    named = member[...]
    part = share[...]
    for first in range(0, TREATIES, BLOCK):
        local = named - first
        inside = (local >= 0) & (local < BLOCK)
        local = jnp.where(inside, local, BLOCK).astype(jnp.float32).astype(jnp.bfloat16)
        for at in range(0, columns, LANES):
            block = zero
            for slot in range(MEMB):
                hit = treaty == local[slot : slot + 1, at : at + LANES]
                block = jnp.where(hit, part[slot : slot + 1, at : at + LANES], block)
            weights[first : first + BLOCK, at : at + LANES] = block
    fetches[2].wait()
    fetches[3].wait()
    fetches[0].wait()
    ceded[...] = clamp_between(
        loss[...].astype(jnp.float32) - retention[...], 0.0, risk_limit[...]
    ).astype(jnp.bfloat16)
    for first in range(0, TREATIES, BLOCK):
        sums[first : first + BLOCK, :] = lax.dot_general(
            weights[first : first + BLOCK, :],
            ceded[...],
            BY_ROWS,
            preferred_element_type=jnp.float32,
        ).astype(jnp.bfloat16)
    fetches[1].wait()
    local_year = jnp.where(year[...] < 0, -1, year[...] & (YEAR_DEV - 1))
    hit = lax.broadcasted_iota(jnp.int32, hits.shape, 0) == local_year
    hits[...] = jnp.where(hit, 1.0, 0.0).astype(jnp.bfloat16)
    for row in range(6):
        fetches[6 + row].wait()
        table[row : row + 1, :] = held[6 + row][...].astype(jnp.float32)


def shard_sums(inputs):
    rows, columns = inputs[0].shape
    count = inputs[6].shape[0]
    views = [
        inputs[0],
        inputs[1].reshape(1, -1),
        inputs[2].reshape(1, -1),
        inputs[3].reshape(1, -1),
        inputs[4].T,
        inputs[5].T,
        *(column.reshape(1, -1) for column in inputs[6:]),
    ]
    views = [pltpu.with_memory_space_constraint(view, pltpu.HBM) for view in views]
    return pl.pallas_call(
        shard_sums_kernel,
        out_shape=(
            jax.ShapeDtypeStruct((TREATIES, rows), jnp.bfloat16),
            jax.ShapeDtypeStruct((8, count), jnp.float32),
            jax.ShapeDtypeStruct((YEAR_DEV, rows), jnp.bfloat16),
        ),
        in_specs=[HBM] * len(views),
        out_specs=(VMEM, VMEM, VMEM),
        scratch_shapes=[
            *(pltpu.VMEM(view.shape, view.dtype) for view in views),
            pltpu.VMEM((TREATIES, columns), jnp.bfloat16),
            pltpu.VMEM((rows, columns), jnp.bfloat16),
            pltpu.SemaphoreType.DMA((len(views),)),
        ],
        compiler_params=PARAMS,
        name="shard_sums",
    )(*views)


def as_column(row):
    count = row.shape[1]
    down = lax.broadcasted_iota(jnp.int32, (count, count), 0)
    across = lax.broadcasted_iota(jnp.int32, (count, count), 1)
    return jnp.sum(jnp.where(down == across, row, 0.0), axis=1, keepdims=True)


def in_two(values):
    high = values.astype(jnp.bfloat16)
    low = (values - high.astype(jnp.float32)).astype(jnp.bfloat16)
    return [high, low]


def annual_kernel(blocks, table, hits, net, kept, sent):
    count = table.shape[1]
    total = blocks[0].astype(jnp.float32)
    for shard in range(1, blocks.shape[0]):
        total = total + blocks[shard].astype(jnp.float32)
    attach = table[0:1, :] * UNIT_LOSS
    limit = table[1:2, :] * UNIT_LOSS
    again = table[2:3, :]
    rate = table[3:4, :]
    recovered = clamp_between(total - as_column(attach), 0.0, as_column(limit))
    retained = total - recovered
    pieces = jnp.concatenate(in_two(recovered) + in_two(retained), axis=0)
    yearly = lax.dot_general(hits[...], pieces, BY_ROWS, preferred_element_type=jnp.float32)
    annual = yearly[:, :count] + yearly[:, count : 2 * count]
    kept_annual = yearly[:, 2 * count : 3 * count] + yearly[:, 3 * count :]
    paid = jnp.minimum(annual, (1.0 + again) * limit)
    net[...] = (paid - rate * jnp.minimum(paid, again * limit)) / limit
    kept[...] = kept_annual
    half = YEAR_DEV // 2
    line = jnp.concatenate((kept_annual[:half], kept_annual[half:]), axis=1)
    for peer in range(sent.shape[0]):
        sent[peer] = line


def annual_tables(blocks, table, hits, peers):
    count = table.shape[1]
    tables = jax.ShapeDtypeStruct((YEAR_DEV, count), jnp.float32)
    return pl.pallas_call(
        annual_kernel,
        out_shape=(
            tables,
            tables,
            jax.ShapeDtypeStruct((peers, YEAR_DEV // 2, 2 * count), jnp.float32),
        ),
        in_specs=[VMEM] * 3,
        out_specs=(VMEM, VMEM, VMEM),
        compiler_params=PARAMS,
        name="annual_tables",
    )(blocks, table, hits)


def exchange(items, low, high):
    items[low], items[high] = (
        jnp.maximum(items[low], items[high]),
        jnp.minimum(items[low], items[high]),
    )


def sort_falling(items):
    count = len(items)
    step = 1
    while step < count:
        gap = step
        while gap >= 1:
            for base in range(gap % step, count - gap, 2 * gap):
                for at in range(base, base + min(gap, count - base - gap)):
                    if at // (2 * step) == (at + gap) // (2 * step):
                        exchange(items, at, at + gap)
            gap //= 2
        step *= 2


def larger_half(first, second):
    return [jnp.maximum(one, two) for one, two in zip(first, reversed(second))]


def sort_bitonic(items):
    gap = len(items) // 2
    while gap >= 1:
        for at in range(len(items)):
            if at & gap == 0:
                exchange(items, at, at + gap)
        gap //= 2


def outcome_kernel(everyone, kept, table, stop_loss, tail_mean):
    peers, rows, lanes = everyone.shape
    count = lanes // 2
    tiles = [
        everyone[peer, at : at + 8, :] for peer in range(peers) for at in range(0, rows, 8)
    ]
    total = tiles[0]
    for tile in tiles[1:]:
        total = total + tile
    summed = jnp.sum(total, axis=0, keepdims=True)
    summed = summed + pltpu.roll(summed, count, 1)
    base_loss = UNIT_LOSS + summed / (peers * YEAR_DEV)
    largest = None
    for at in range(0, len(tiles), TAIL):
        group = tiles[at : at + TAIL]
        sort_falling(group)
        if largest is None:
            largest = group
        else:
            largest = larger_half(largest, group)
            sort_bitonic(largest)
    for shift in (4, 2, 1):
        largest = larger_half(largest, [pltpu.roll(item, shift, 0) for item in largest])
        sort_bitonic(largest)
    largest = larger_half(largest, [pltpu.roll(item, count, 1) for item in largest])
    top = largest[0]
    for item in largest[1:]:
        top = top + item
    tail_mean[...] = (top[0:1, :] / base_loss / TAIL)[:, :count]
    stop_loss[...] = clamp_between(
        kept[...] / base_loss[:, :count] - table[4:5, :], 0.0, table[5:6, :]
    )


def outcomes(everyone, kept, table):
    return pl.pallas_call(
        outcome_kernel,
        out_shape=(
            jax.ShapeDtypeStruct(kept.shape, jnp.float32),
            jax.ShapeDtypeStruct((1, kept.shape[1]), jnp.float32),
        ),
        in_specs=[VMEM] * 3,
        out_specs=(VMEM, VMEM),
        compiler_params=PARAMS,
        name="outcomes",
    )(everyone, kept, table)


def on_device(*inputs):
    ports = lax.axis_size("port")
    sums, table, hits = shard_sums(inputs)
    blocks = lax.all_to_all(
        sums.reshape(ports, -1, sums.shape[1]), "port", 0, 0, tiled=True
    )
    net, kept, sent = annual_tables(blocks, table, hits, lax.axis_size("year"))
    everyone = lax.all_to_all(sent, "year", 0, 0, tiled=True)
    stop_loss, tail_mean = outcomes(everyone, kept, table)
    return (net.T, stop_loss.T, tail_mean.reshape(-1))


def solution(mesh):
    return jax.shard_map(
        on_device,
        mesh=mesh,
        in_specs=(
            P("year", "port"),
            P("year"),
            P("port"),
            P("port"),
            P("port", None),
            P("port", None),
            P("port"),
            P("port"),
            P("port"),
            P("port"),
            P("port"),
            P("port"),
        ),
        out_specs=(P("port", "year"), P("port", "year"), P("port")),
        check_vma=False,
    )
```

```python
import jax
import jax.numpy as jnp
from jax import lax
from jax.experimental import pallas as pl
from jax.experimental.pallas import tpu as pltpu
from jax.sharding import PartitionSpec as P

TREATIES = 1024
MEMB = 4
YEAR_DEV = 32
TAIL = 16
LANES = 128
BLOCK = 256

UNIT_LOSS = 1.0

VMEM = pl.BlockSpec(memory_space=pltpu.VMEM)
HBM = pl.BlockSpec(memory_space=pltpu.HBM)
PARAMS = pltpu.CompilerParams(vmem_limit_bytes=16 * 1024 * 1024)
BY_ROWS = (((1,), (1,)), ((), ()))


def clamp_between(values, lower, upper):
    return jnp.minimum(jnp.maximum(values, lower), upper)


def shard_sums_kernel(*refs):
    inputs, (sums, table, hits), held = refs[:12], refs[12:15], refs[15:27]
    weights, ceded, arrived = refs[27:]
    order = (5, 4, 2, 3, 0, 1, 6, 7, 8, 9, 10, 11)
    fetches = {
        k: pltpu.make_async_copy(inputs[k], held[k], arrived.at[k]) for k in order
    }
    for k in order:
        fetches[k].start()
    loss, year, retention, risk_limit, share, member = held[:6]
    columns = loss.shape[1]
    treaty = lax.broadcasted_iota(jnp.int32, (BLOCK, LANES), 0)
    treaty = treaty.astype(jnp.float32).astype(jnp.bfloat16)
    zero = jnp.zeros((BLOCK, LANES), jnp.bfloat16)
    fetches[5].wait()
    fetches[4].wait()
    named = member[...]
    part = share[...]

    def build(first):
        local = named - first
        inside = (local >= 0) & (local < BLOCK)
        local = jnp.where(inside, local, BLOCK).astype(jnp.float32).astype(jnp.bfloat16)
        for at in range(0, columns, LANES):
            block = zero
            for slot in range(MEMB):
                hit = treaty == local[slot : slot + 1, at : at + LANES]
                block = jnp.where(hit, part[slot : slot + 1, at : at + LANES], block)
            weights[first : first + BLOCK, at : at + LANES] = block

    def multiply(first):
        sums[first : first + BLOCK, :] = lax.dot_general(
            weights[first : first + BLOCK, :],
            ceded[...],
            BY_ROWS,
            preferred_element_type=jnp.float32,
        ).astype(jnp.bfloat16)

    blocks = list(range(0, TREATIES, BLOCK))
    ahead = 2
    for first in blocks[:ahead]:
        build(first)
    fetches[2].wait()
    fetches[3].wait()
    fetches[0].wait()
    ceded[...] = clamp_between(
        loss[...].astype(jnp.float32) - retention[...], 0.0, risk_limit[...]
    ).astype(jnp.bfloat16)
    for k, first in enumerate(blocks):
        multiply(first)
        if k + ahead < len(blocks):
            build(blocks[k + ahead])
    fetches[1].wait()
    local_year = jnp.where(year[...] < 0, -1, year[...] & (YEAR_DEV - 1))
    hit = lax.broadcasted_iota(jnp.int32, hits.shape, 0) == local_year
    hits[...] = jnp.where(hit, 1.0, 0.0).astype(jnp.bfloat16)
    for row in range(6):
        fetches[6 + row].wait()
        table[row : row + 1, :] = held[6 + row][...].astype(jnp.float32)


def shard_sums(inputs):
    rows, columns = inputs[0].shape
    count = inputs[6].shape[0]
    views = [
        inputs[0],
        inputs[1].reshape(1, -1),
        inputs[2].reshape(1, -1),
        inputs[3].reshape(1, -1),
        inputs[4].T,
        inputs[5].T,
        *(column.reshape(1, -1) for column in inputs[6:]),
    ]
    views = [pltpu.with_memory_space_constraint(view, pltpu.HBM) for view in views]
    return pl.pallas_call(
        shard_sums_kernel,
        out_shape=(
            jax.ShapeDtypeStruct((TREATIES, rows), jnp.bfloat16),
            jax.ShapeDtypeStruct((8, count), jnp.float32),
            jax.ShapeDtypeStruct((YEAR_DEV, rows), jnp.bfloat16),
        ),
        in_specs=[HBM] * len(views),
        out_specs=(VMEM, VMEM, VMEM),
        scratch_shapes=[
            *(pltpu.VMEM(view.shape, view.dtype) for view in views),
            pltpu.VMEM((TREATIES, columns), jnp.bfloat16),
            pltpu.VMEM((rows, columns), jnp.bfloat16),
            pltpu.SemaphoreType.DMA((len(views),)),
        ],
        compiler_params=PARAMS,
        name="shard_sums",
    )(*views)


def as_column(row):
    count = row.shape[1]
    down = lax.broadcasted_iota(jnp.int32, (count, count), 0)
    across = lax.broadcasted_iota(jnp.int32, (count, count), 1)
    return jnp.sum(jnp.where(down == across, row, 0.0), axis=1, keepdims=True)


def in_two(values):
    high = values.astype(jnp.bfloat16)
    low = (values - high.astype(jnp.float32)).astype(jnp.bfloat16)
    return [high, low]


def annual_kernel(blocks, table, hits, annual, kept, sent):
    count = table.shape[1]
    total = blocks[0].astype(jnp.float32)
    for shard in range(1, blocks.shape[0]):
        total = total + blocks[shard].astype(jnp.float32)
    attach = table[0:1, :] * UNIT_LOSS
    limit = table[1:2, :] * UNIT_LOSS
    recovered = clamp_between(total - as_column(attach), 0.0, as_column(limit))
    retained = total - recovered
    pieces = jnp.concatenate(in_two(recovered) + in_two(retained), axis=0)
    yearly = lax.dot_general(hits[...], pieces, BY_ROWS, preferred_element_type=jnp.float32)
    annual[...] = yearly[:, :count] + yearly[:, count : 2 * count]
    kept_annual = yearly[:, 2 * count : 3 * count] + yearly[:, 3 * count :]
    kept[...] = kept_annual
    half = YEAR_DEV // 2
    line = jnp.concatenate((kept_annual[:half], kept_annual[half:]), axis=1)
    for peer in range(sent.shape[0]):
        sent[peer] = line


def annual_tables(blocks, table, hits, peers):
    count = table.shape[1]
    tables = jax.ShapeDtypeStruct((YEAR_DEV, count), jnp.float32)
    return pl.pallas_call(
        annual_kernel,
        out_shape=(
            tables,
            tables,
            jax.ShapeDtypeStruct((peers, YEAR_DEV // 2, 2 * count), jnp.float32),
        ),
        in_specs=[VMEM] * 3,
        out_specs=(VMEM, VMEM, VMEM),
        compiler_params=PARAMS,
        name="annual_tables",
    )(blocks, table, hits)


def exchange(items, low, high):
    items[low], items[high] = (
        jnp.maximum(items[low], items[high]),
        jnp.minimum(items[low], items[high]),
    )


def sort_falling(items):
    count = len(items)
    step = 1
    while step < count:
        gap = step
        while gap >= 1:
            for base in range(gap % step, count - gap, 2 * gap):
                for at in range(base, base + min(gap, count - base - gap)):
                    if at // (2 * step) == (at + gap) // (2 * step):
                        exchange(items, at, at + gap)
            gap //= 2
        step *= 2


def larger_half(first, second):
    return [jnp.maximum(one, two) for one, two in zip(first, reversed(second))]


def sort_bitonic(items):
    gap = len(items) // 2
    while gap >= 1:
        for at in range(len(items)):
            if at & gap == 0:
                exchange(items, at, at + gap)
        gap //= 2


def outcome_kernel(everyone, annual, kept, table, net, stop_loss, tail_mean):
    limit = table[1:2, :] * UNIT_LOSS
    again = table[2:3, :]
    rate = table[3:4, :]
    paid = jnp.minimum(annual[...], (1.0 + again) * limit)
    net[...] = (paid - rate * jnp.minimum(paid, again * limit)) / limit
    peers, rows, lanes = everyone.shape
    count = lanes // 2
    tiles = [
        everyone[peer, at : at + 8, :] for peer in range(peers) for at in range(0, rows, 8)
    ]
    total = tiles[0]
    for tile in tiles[1:]:
        total = total + tile
    summed = jnp.sum(total, axis=0, keepdims=True)
    summed = summed + pltpu.roll(summed, count, 1)
    base_loss = UNIT_LOSS + summed / (peers * YEAR_DEV)
    largest = None
    for at in range(0, len(tiles), TAIL):
        group = tiles[at : at + TAIL]
        sort_falling(group)
        if largest is None:
            largest = group
        else:
            largest = larger_half(largest, group)
            sort_bitonic(largest)
    for shift in (4, 2, 1):
        largest = larger_half(largest, [pltpu.roll(item, shift, 0) for item in largest])
        sort_bitonic(largest)
    largest = larger_half(largest, [pltpu.roll(item, count, 1) for item in largest])
    top = largest[0]
    for item in largest[1:]:
        top = top + item
    tail_mean[...] = (top[0:1, :] / base_loss / TAIL)[:, :count]
    stop_loss[...] = clamp_between(
        kept[...] / base_loss[:, :count] - table[4:5, :], 0.0, table[5:6, :]
    )


def outcomes(everyone, annual, kept, table):
    return pl.pallas_call(
        outcome_kernel,
        out_shape=(
            jax.ShapeDtypeStruct(kept.shape, jnp.float32),
            jax.ShapeDtypeStruct(kept.shape, jnp.float32),
            jax.ShapeDtypeStruct((1, kept.shape[1]), jnp.float32),
        ),
        in_specs=[VMEM] * 4,
        out_specs=(VMEM, VMEM, VMEM),
        compiler_params=PARAMS,
        name="outcomes",
    )(everyone, annual, kept, table)


def on_device(*inputs):
    ports = lax.axis_size("port")
    sums, table, hits = shard_sums(inputs)
    blocks = lax.all_to_all(
        sums.reshape(ports, -1, sums.shape[1]), "port", 0, 0, tiled=True
    )
    annual, kept, sent = annual_tables(blocks, table, hits, lax.axis_size("year"))
    everyone = lax.all_to_all(sent, "year", 0, 0, tiled=True)
    net, stop_loss, tail_mean = outcomes(everyone, annual, kept, table)
    return (net.T, stop_loss.T, tail_mean.reshape(-1))


def solution(mesh):
    return jax.shard_map(
        on_device,
        mesh=mesh,
        in_specs=(
            P("year", "port"),
            P("year"),
            P("port"),
            P("port"),
            P("port", None),
            P("port", None),
            P("port"),
            P("port"),
            P("port"),
            P("port"),
            P("port"),
            P("port"),
        ),
        out_specs=(P("port", "year"), P("port", "year"), P("port")),
        check_vma=False,
    )
```

```python
import jax
import jax.numpy as jnp
from jax import lax
from jax.experimental import pallas as pl
from jax.experimental.pallas import tpu as pltpu
from jax.sharding import PartitionSpec as P

TREATIES = 1024
MEMB = 4
YEAR_DEV = 32
TAIL = 16
LANES = 128
BLOCK = 256

UNIT_LOSS = 1.0

VMEM = pl.BlockSpec(memory_space=pltpu.VMEM)
HBM = pl.BlockSpec(memory_space=pltpu.HBM)
PARAMS = pltpu.CompilerParams(vmem_limit_bytes=16 * 1024 * 1024)
BY_ROWS = (((1,), (1,)), ((), ()))


def clamp_between(values, lower, upper):
    return jnp.minimum(jnp.maximum(values, lower), upper)


def shard_sums_kernel(*refs):
    inputs, (sums, table, hits), held = refs[:12], refs[12:15], refs[15:27]
    weights, ceded, arrived = refs[27:]
    order = (5, 4, 2, 3, 0, 1, 6, 7, 8, 9, 10, 11)
    fetches = {
        k: pltpu.make_async_copy(inputs[k], held[k], arrived.at[k]) for k in order
    }
    for k in order:
        fetches[k].start()
    loss, year, retention, risk_limit, share, member = held[:6]
    columns = loss.shape[1]
    treaty = lax.broadcasted_iota(jnp.int32, (BLOCK, LANES), 0)
    treaty = treaty.astype(jnp.float32).astype(jnp.bfloat16)
    zero = jnp.zeros((BLOCK, LANES), jnp.bfloat16)
    fetches[5].wait()
    fetches[4].wait()
    named = member[...]
    part = share[...]

    def build(first):
        local = named - first
        inside = (local >= 0) & (local < BLOCK)
        local = jnp.where(inside, local, BLOCK).astype(jnp.float32).astype(jnp.bfloat16)
        for at in range(0, columns, LANES):
            block = zero
            for slot in range(MEMB):
                hit = treaty == local[slot : slot + 1, at : at + LANES]
                block = jnp.where(hit, part[slot : slot + 1, at : at + LANES], block)
            weights[first : first + BLOCK, at : at + LANES] = block

    def multiply(first):
        sums[first : first + BLOCK, :] = lax.dot_general(
            weights[first : first + BLOCK, :],
            ceded[...],
            BY_ROWS,
            preferred_element_type=jnp.float32,
        ).astype(jnp.bfloat16)

    blocks = list(range(0, TREATIES, BLOCK))
    ahead = 2
    for first in blocks[:ahead]:
        build(first)
    fetches[2].wait()
    fetches[3].wait()
    fetches[0].wait()
    ceded[...] = clamp_between(
        loss[...].astype(jnp.float32) - retention[...], 0.0, risk_limit[...]
    ).astype(jnp.bfloat16)
    for k, first in enumerate(blocks):
        multiply(first)
        if k + ahead < len(blocks):
            build(blocks[k + ahead])
    fetches[1].wait()
    local_year = jnp.where(year[...] < 0, -1, year[...] & (YEAR_DEV - 1))
    hit = lax.broadcasted_iota(jnp.int32, hits.shape, 0) == local_year
    hits[...] = jnp.where(hit, 1.0, 0.0).astype(jnp.bfloat16)
    for row in range(6):
        fetches[6 + row].wait()
        table[row : row + 1, :] = held[6 + row][...].astype(jnp.float32)


def shard_sums(inputs):
    rows, columns = inputs[0].shape
    count = inputs[6].shape[0]
    views = [
        inputs[0],
        inputs[1].reshape(1, -1),
        inputs[2].reshape(1, -1),
        inputs[3].reshape(1, -1),
        inputs[4].T,
        inputs[5].T,
        *(column.reshape(1, -1) for column in inputs[6:]),
    ]
    views = [pltpu.with_memory_space_constraint(view, pltpu.HBM) for view in views]
    return pl.pallas_call(
        shard_sums_kernel,
        out_shape=(
            jax.ShapeDtypeStruct((TREATIES, rows), jnp.bfloat16),
            jax.ShapeDtypeStruct((8, count), jnp.float32),
            jax.ShapeDtypeStruct((YEAR_DEV, rows), jnp.bfloat16),
        ),
        in_specs=[HBM] * len(views),
        out_specs=(VMEM, VMEM, VMEM),
        scratch_shapes=[
            *(pltpu.VMEM(view.shape, view.dtype) for view in views),
            pltpu.VMEM((TREATIES, columns), jnp.bfloat16),
            pltpu.VMEM((rows, columns), jnp.bfloat16),
            pltpu.SemaphoreType.DMA((len(views),)),
        ],
        compiler_params=PARAMS,
        name="shard_sums",
    )(*views)


def as_column(row):
    count = row.shape[1]
    down = lax.broadcasted_iota(jnp.int32, (count, count), 0)
    across = lax.broadcasted_iota(jnp.int32, (count, count), 1)
    return jnp.sum(jnp.where(down == across, row, 0.0), axis=1, keepdims=True)


def in_two(values):
    high = values.astype(jnp.bfloat16)
    low = (values - high.astype(jnp.float32)).astype(jnp.bfloat16)
    return [high, low]


def annual_kernel(blocks, table, hits, annual, kept, sent):
    count = table.shape[1]
    total = blocks[0].astype(jnp.float32)
    for shard in range(1, blocks.shape[0]):
        total = total + blocks[shard].astype(jnp.float32)
    attach = table[0:1, :] * UNIT_LOSS
    limit = table[1:2, :] * UNIT_LOSS
    recovered = clamp_between(total - as_column(attach), 0.0, as_column(limit))
    retained = total - recovered
    pieces = jnp.concatenate(in_two(recovered) + in_two(retained), axis=0)
    yearly = lax.dot_general(hits[...], pieces, BY_ROWS, preferred_element_type=jnp.float32)
    annual[...] = yearly[:, :count] + yearly[:, count : 2 * count]
    kept_annual = yearly[:, 2 * count : 3 * count] + yearly[:, 3 * count :]
    kept[...] = kept_annual
    half = YEAR_DEV // 2
    line = jnp.concatenate((kept_annual[:half], kept_annual[half:]), axis=1)
    line = line.astype(jnp.bfloat16)
    for peer in range(sent.shape[0]):
        sent[peer] = line


def annual_tables(blocks, table, hits, peers):
    count = table.shape[1]
    tables = jax.ShapeDtypeStruct((YEAR_DEV, count), jnp.float32)
    return pl.pallas_call(
        annual_kernel,
        out_shape=(
            tables,
            tables,
            jax.ShapeDtypeStruct((peers, YEAR_DEV // 2, 2 * count), jnp.bfloat16),
        ),
        in_specs=[VMEM] * 3,
        out_specs=(VMEM, VMEM, VMEM),
        compiler_params=PARAMS,
        name="annual_tables",
    )(blocks, table, hits)


def exchange(items, low, high):
    items[low], items[high] = (
        jnp.maximum(items[low], items[high]),
        jnp.minimum(items[low], items[high]),
    )


def sort_falling(items):
    count = len(items)
    step = 1
    while step < count:
        gap = step
        while gap >= 1:
            for base in range(gap % step, count - gap, 2 * gap):
                for at in range(base, base + min(gap, count - base - gap)):
                    if at // (2 * step) == (at + gap) // (2 * step):
                        exchange(items, at, at + gap)
            gap //= 2
        step *= 2


def larger_half(first, second):
    return [jnp.maximum(one, two) for one, two in zip(first, reversed(second))]


def sort_bitonic(items):
    gap = len(items) // 2
    while gap >= 1:
        for at in range(len(items)):
            if at & gap == 0:
                exchange(items, at, at + gap)
        gap //= 2


def outcome_kernel(everyone, annual, kept, table, net, stop_loss, tail_mean):
    limit = table[1:2, :] * UNIT_LOSS
    again = table[2:3, :]
    rate = table[3:4, :]
    paid = jnp.minimum(annual[...], (1.0 + again) * limit)
    net[...] = (paid - rate * jnp.minimum(paid, again * limit)) / limit
    peers, rows, lanes = everyone.shape
    count = lanes // 2
    tiles = [
        line[at : at + 8, :]
        for line in (everyone[peer].astype(jnp.float32) for peer in range(peers))
        for at in range(0, rows, 8)
    ]
    total = tiles[0]
    for tile in tiles[1:]:
        total = total + tile
    summed = jnp.sum(total, axis=0, keepdims=True)
    summed = summed + pltpu.roll(summed, count, 1)
    base_loss = UNIT_LOSS + summed / (peers * YEAR_DEV)
    largest = None
    for at in range(0, len(tiles), TAIL):
        group = tiles[at : at + TAIL]
        sort_falling(group)
        if largest is None:
            largest = group
        else:
            largest = larger_half(largest, group)
            sort_bitonic(largest)
    for shift in (4, 2, 1):
        largest = larger_half(largest, [pltpu.roll(item, shift, 0) for item in largest])
        sort_bitonic(largest)
    largest = larger_half(largest, [pltpu.roll(item, count, 1) for item in largest])
    top = largest[0]
    for item in largest[1:]:
        top = top + item
    tail_mean[...] = (top[0:1, :] / base_loss / TAIL)[:, :count]
    stop_loss[...] = clamp_between(
        kept[...] / base_loss[:, :count] - table[4:5, :], 0.0, table[5:6, :]
    )


def outcomes(everyone, annual, kept, table):
    return pl.pallas_call(
        outcome_kernel,
        out_shape=(
            jax.ShapeDtypeStruct(kept.shape, jnp.float32),
            jax.ShapeDtypeStruct(kept.shape, jnp.float32),
            jax.ShapeDtypeStruct((1, kept.shape[1]), jnp.float32),
        ),
        in_specs=[VMEM] * 4,
        out_specs=(VMEM, VMEM, VMEM),
        compiler_params=PARAMS,
        name="outcomes",
    )(everyone, annual, kept, table)


def on_device(*inputs):
    ports = lax.axis_size("port")
    sums, table, hits = shard_sums(inputs)
    blocks = lax.all_to_all(
        sums.reshape(ports, -1, sums.shape[1]), "port", 0, 0, tiled=True
    )
    annual, kept, sent = annual_tables(blocks, table, hits, lax.axis_size("year"))
    everyone = lax.all_to_all(sent, "year", 0, 0, tiled=True)
    net, stop_loss, tail_mean = outcomes(everyone, annual, kept, table)
    return (net.T, stop_loss.T, tail_mean.reshape(-1))


def solution(mesh):
    return jax.shard_map(
        on_device,
        mesh=mesh,
        in_specs=(
            P("year", "port"),
            P("year"),
            P("port"),
            P("port"),
            P("port", None),
            P("port", None),
            P("port"),
            P("port"),
            P("port"),
            P("port"),
            P("port"),
            P("port"),
        ),
        out_specs=(P("port", "year"), P("port", "year"), P("port")),
        check_vma=False,
    )
```

```python
import jax
import jax.numpy as jnp
from jax import lax
from jax.experimental import pallas as pl
from jax.experimental.pallas import tpu as pltpu
from jax.sharding import PartitionSpec as P

TREATIES = 1024
MEMB = 4
YEAR_DEV = 32
TAIL = 16
LANES = 128
BLOCK = 256

UNIT_LOSS = 1.0

VMEM = pl.BlockSpec(memory_space=pltpu.VMEM)
SMEM = pl.BlockSpec(memory_space=pltpu.SMEM)
HBM = pl.BlockSpec(memory_space=pltpu.HBM)
PARAMS = pltpu.CompilerParams(vmem_limit_bytes=16 * 1024 * 1024)
BY_ROWS = (((1,), (1,)), ((), ()))


def clamp_between(values, lower, upper):
    return jnp.minimum(jnp.maximum(values, lower), upper)


def shard_sums_kernel(*refs):
    inputs, outputs, held = refs[:12], refs[12:17], refs[17:29]
    sums, first_sums, table, hits, short = outputs
    weights, ceded, arrived = refs[29:]
    order = (5, 4, 2, 3, 0, 1, 6, 7, 8, 9, 10, 11)
    fetches = {
        k: pltpu.make_async_copy(inputs[k], held[k], arrived.at[k]) for k in order
    }
    for k in order:
        fetches[k].start()
    loss, year, retention, risk_limit, share, member = held[:6]
    columns = loss.shape[1]
    treaty = lax.broadcasted_iota(jnp.int32, (BLOCK, LANES), 0)
    treaty = treaty.astype(jnp.float32).astype(jnp.bfloat16)
    zero = jnp.zeros((BLOCK, LANES), jnp.bfloat16)
    fetches[5].wait()
    fetches[4].wait()
    named = member[...]
    part = share[...]

    def build(first):
        local = named - first
        inside = (local >= 0) & (local < BLOCK)
        local = jnp.where(inside, local, BLOCK).astype(jnp.float32).astype(jnp.bfloat16)
        for at in range(0, columns, LANES):
            block = zero
            for slot in range(MEMB):
                hit = treaty == local[slot : slot + 1, at : at + LANES]
                block = jnp.where(hit, part[slot : slot + 1, at : at + LANES], block)
            weights[first : first + BLOCK, at : at + LANES] = block

    def multiply(first):
        block = lax.dot_general(
            weights[first : first + BLOCK, :],
            ceded[...],
            BY_ROWS,
            preferred_element_type=jnp.float32,
        ).astype(jnp.bfloat16)
        sums[first : first + BLOCK, :] = block
        first_sums[first : first + BLOCK, :] = block[:, : first_sums.shape[1]]

    blocks = list(range(0, TREATIES, BLOCK))
    ahead = 2
    for first in blocks[:ahead]:
        build(first)
    fetches[2].wait()
    fetches[3].wait()
    fetches[0].wait()
    ceded[...] = clamp_between(
        loss[...].astype(jnp.float32) - retention[...], 0.0, risk_limit[...]
    ).astype(jnp.bfloat16)
    for k, first in enumerate(blocks):
        multiply(first)
        if k + ahead < len(blocks):
            build(blocks[k + ahead])
    fetches[1].wait()
    local_year = jnp.where(year[...] < 0, -1, year[...] & (YEAR_DEV - 1))
    hit = lax.broadcasted_iota(jnp.int32, hits.shape, 0) == local_year
    hits[...] = jnp.where(hit, 1.0, 0.0).astype(jnp.bfloat16)
    late = lax.broadcasted_iota(jnp.int32, year.shape, 1) >= first_sums.shape[1]
    short[0] = 1 - jnp.max(jnp.where(late & (year[...] >= 0), 1, 0))
    for row in range(6):
        fetches[6 + row].wait()
        table[row : row + 1, :] = held[6 + row][...].astype(jnp.float32)


def shard_sums(inputs):
    rows, columns = inputs[0].shape
    count = inputs[6].shape[0]
    views = [
        inputs[0],
        inputs[1].reshape(1, -1),
        inputs[2].reshape(1, -1),
        inputs[3].reshape(1, -1),
        inputs[4].T,
        inputs[5].T,
        *(column.reshape(1, -1) for column in inputs[6:]),
    ]
    views = [pltpu.with_memory_space_constraint(view, pltpu.HBM) for view in views]
    return pl.pallas_call(
        shard_sums_kernel,
        out_shape=(
            jax.ShapeDtypeStruct((TREATIES, rows), jnp.bfloat16),
            jax.ShapeDtypeStruct((TREATIES, rows // 2), jnp.bfloat16),
            jax.ShapeDtypeStruct((8, count), jnp.float32),
            jax.ShapeDtypeStruct((YEAR_DEV, rows), jnp.bfloat16),
            jax.ShapeDtypeStruct((1,), jnp.int32),
        ),
        in_specs=[HBM] * len(views),
        out_specs=(VMEM, VMEM, VMEM, VMEM, SMEM),
        scratch_shapes=[
            *(pltpu.VMEM(view.shape, view.dtype) for view in views),
            pltpu.VMEM((TREATIES, columns), jnp.bfloat16),
            pltpu.VMEM((rows, columns), jnp.bfloat16),
            pltpu.SemaphoreType.DMA((len(views),)),
        ],
        compiler_params=PARAMS,
        name="shard_sums",
    )(*views)


def as_column(row):
    count = row.shape[1]
    down = lax.broadcasted_iota(jnp.int32, (count, count), 0)
    across = lax.broadcasted_iota(jnp.int32, (count, count), 1)
    return jnp.sum(jnp.where(down == across, row, 0.0), axis=1, keepdims=True)


def in_two(values):
    high = values.astype(jnp.bfloat16)
    low = (values - high.astype(jnp.float32)).astype(jnp.bfloat16)
    return [high, low]


def annual_kernel(blocks, table, hits, annual, kept, sent):
    count = table.shape[1]
    total = blocks[0].astype(jnp.float32)
    for shard in range(1, blocks.shape[0]):
        total = total + blocks[shard].astype(jnp.float32)
    attach = table[0:1, :] * UNIT_LOSS
    limit = table[1:2, :] * UNIT_LOSS
    recovered = clamp_between(total - as_column(attach), 0.0, as_column(limit))
    retained = total - recovered
    pieces = jnp.concatenate(in_two(recovered) + in_two(retained), axis=0)
    yearly = lax.dot_general(
        hits[:, : total.shape[1]], pieces, BY_ROWS, preferred_element_type=jnp.float32
    )
    annual[...] = yearly[:, :count] + yearly[:, count : 2 * count]
    kept_annual = yearly[:, 2 * count : 3 * count] + yearly[:, 3 * count :]
    kept[...] = kept_annual
    half = YEAR_DEV // 2
    line = jnp.concatenate((kept_annual[:half], kept_annual[half:]), axis=1)
    line = line.astype(jnp.bfloat16)
    for peer in range(sent.shape[0]):
        sent[peer] = line


def annual_tables(blocks, table, hits, peers):
    count = table.shape[1]
    tables = jax.ShapeDtypeStruct((YEAR_DEV, count), jnp.float32)
    return pl.pallas_call(
        annual_kernel,
        out_shape=(
            tables,
            tables,
            jax.ShapeDtypeStruct((peers, YEAR_DEV // 2, 2 * count), jnp.bfloat16),
        ),
        in_specs=[VMEM] * 3,
        out_specs=(VMEM, VMEM, VMEM),
        compiler_params=PARAMS,
        name="annual_tables",
    )(blocks, table, hits)


def exchange(items, low, high):
    items[low], items[high] = (
        jnp.maximum(items[low], items[high]),
        jnp.minimum(items[low], items[high]),
    )


def sort_falling(items):
    count = len(items)
    step = 1
    while step < count:
        gap = step
        while gap >= 1:
            for base in range(gap % step, count - gap, 2 * gap):
                for at in range(base, base + min(gap, count - base - gap)):
                    if at // (2 * step) == (at + gap) // (2 * step):
                        exchange(items, at, at + gap)
            gap //= 2
        step *= 2


def larger_half(first, second):
    return [jnp.maximum(one, two) for one, two in zip(first, reversed(second))]


def sort_bitonic(items):
    gap = len(items) // 2
    while gap >= 1:
        for at in range(len(items)):
            if at & gap == 0:
                exchange(items, at, at + gap)
        gap //= 2


def outcome_kernel(everyone, annual, kept, table, net, stop_loss, tail_mean):
    limit = table[1:2, :] * UNIT_LOSS
    again = table[2:3, :]
    rate = table[3:4, :]
    paid = jnp.minimum(annual[...], (1.0 + again) * limit)
    net[...] = (paid - rate * jnp.minimum(paid, again * limit)) / limit
    peers, rows, lanes = everyone.shape
    count = lanes // 2
    tiles = [
        line[at : at + 8, :]
        for line in (everyone[peer].astype(jnp.float32) for peer in range(peers))
        for at in range(0, rows, 8)
    ]
    total = tiles[0]
    for tile in tiles[1:]:
        total = total + tile
    summed = jnp.sum(total, axis=0, keepdims=True)
    summed = summed + pltpu.roll(summed, count, 1)
    base_loss = UNIT_LOSS + summed / (peers * YEAR_DEV)
    largest = None
    for at in range(0, len(tiles), TAIL):
        group = tiles[at : at + TAIL]
        sort_falling(group)
        if largest is None:
            largest = group
        else:
            largest = larger_half(largest, group)
            sort_bitonic(largest)
    for shift in (4, 2, 1):
        largest = larger_half(largest, [pltpu.roll(item, shift, 0) for item in largest])
        sort_bitonic(largest)
    largest = larger_half(largest, [pltpu.roll(item, count, 1) for item in largest])
    top = largest[0]
    for item in largest[1:]:
        top = top + item
    tail_mean[...] = (top[0:1, :] / base_loss / TAIL)[:, :count]
    stop_loss[...] = clamp_between(
        kept[...] / base_loss[:, :count] - table[4:5, :], 0.0, table[5:6, :]
    )


def outcomes(everyone, annual, kept, table):
    return pl.pallas_call(
        outcome_kernel,
        out_shape=(
            jax.ShapeDtypeStruct(kept.shape, jnp.float32),
            jax.ShapeDtypeStruct(kept.shape, jnp.float32),
            jax.ShapeDtypeStruct((1, kept.shape[1]), jnp.float32),
        ),
        in_specs=[VMEM] * 4,
        out_specs=(VMEM, VMEM, VMEM),
        compiler_params=PARAMS,
        name="outcomes",
    )(everyone, annual, kept, table)


def on_device(*inputs):
    ports = lax.axis_size("port")
    years = lax.axis_size("year")
    sums, first_sums, table, hits, short = shard_sums(inputs)

    def exchanged(rows):
        blocks = lax.all_to_all(
            rows.reshape(ports, -1, rows.shape[1]), "port", 0, 0, tiled=True
        )
        return annual_tables(blocks, table, hits, years)

    annual, kept, sent = lax.cond(
        short[0] == 1, lambda: exchanged(first_sums), lambda: exchanged(sums)
    )
    everyone = lax.all_to_all(sent, "year", 0, 0, tiled=True)
    net, stop_loss, tail_mean = outcomes(everyone, annual, kept, table)
    return (net.T, stop_loss.T, tail_mean.reshape(-1))


def solution(mesh):
    return jax.shard_map(
        on_device,
        mesh=mesh,
        in_specs=(
            P("year", "port"),
            P("year"),
            P("port"),
            P("port"),
            P("port", None),
            P("port", None),
            P("port"),
            P("port"),
            P("port"),
            P("port"),
            P("port"),
            P("port"),
        ),
        out_specs=(P("port", "year"), P("port", "year"), P("port")),
        check_vma=False,
    )
```

```python
import jax
import jax.numpy as jnp
from jax import lax
from jax.experimental import pallas as pl
from jax.experimental.pallas import tpu as pltpu
from jax.sharding import PartitionSpec as P

TREATIES = 1024
MEMB = 4
YEAR_DEV = 32
TAIL = 16
LANES = 128
BLOCK = 256

UNIT_LOSS = 1.0

VMEM = pl.BlockSpec(memory_space=pltpu.VMEM)
SMEM = pl.BlockSpec(memory_space=pltpu.SMEM)
HBM = pl.BlockSpec(memory_space=pltpu.HBM)
PARAMS = pltpu.CompilerParams(vmem_limit_bytes=16 * 1024 * 1024)
BY_ROWS = (((1,), (1,)), ((), ()))


def clamp_between(values, lower, upper):
    return jnp.minimum(jnp.maximum(values, lower), upper)


def shard_sums_kernel(*refs):
    inputs, outputs, held = refs[:12], refs[12:17], refs[17:29]
    sums, first_sums, table, hits, short = outputs
    weights, ceded, arrived = refs[29:]
    order = (5, 4, 2, 3, 0, 1, 6, 7, 8, 9, 10, 11)
    fetches = {
        k: pltpu.make_async_copy(inputs[k], held[k], arrived.at[k]) for k in order
    }
    for k in order:
        fetches[k].start()
    loss, year, retention, risk_limit, share, member = held[:6]
    columns = loss.shape[1]
    treaty = lax.broadcasted_iota(jnp.int32, (BLOCK, LANES), 0)
    treaty = treaty.astype(jnp.float32).astype(jnp.bfloat16)
    zero = jnp.zeros((BLOCK, LANES), jnp.bfloat16)
    fetches[5].wait()
    fetches[4].wait()
    named = member[...]
    part = share[...]

    def build(first):
        local = named - first
        inside = (local >= 0) & (local < BLOCK)
        local = jnp.where(inside, local, BLOCK).astype(jnp.float32).astype(jnp.bfloat16)
        for at in range(0, columns, LANES):
            block = zero
            for slot in range(MEMB):
                hit = treaty == local[slot : slot + 1, at : at + LANES]
                block = jnp.where(hit, part[slot : slot + 1, at : at + LANES], block)
            weights[first : first + BLOCK, at : at + LANES] = block

    def multiply(first):
        block = lax.dot_general(
            weights[first : first + BLOCK, :],
            ceded[...],
            BY_ROWS,
            preferred_element_type=jnp.float32,
        ).astype(jnp.bfloat16)
        sums[first : first + BLOCK, :] = block
        first_sums[first : first + BLOCK, :] = block[:, : first_sums.shape[1]]

    blocks = list(range(0, TREATIES, BLOCK))
    ahead = 2
    for first in blocks[:ahead]:
        build(first)
    fetches[2].wait()
    fetches[3].wait()
    fetches[0].wait()
    ceded[...] = clamp_between(
        loss[...].astype(jnp.float32) - retention[...], 0.0, risk_limit[...]
    ).astype(jnp.bfloat16)
    for k, first in enumerate(blocks):
        multiply(first)
        if k + ahead < len(blocks):
            build(blocks[k + ahead])
    fetches[1].wait()
    local_year = jnp.where(year[...] < 0, -1, year[...] & (YEAR_DEV - 1))
    hit = lax.broadcasted_iota(jnp.int32, hits.shape, 0) == local_year
    hits[...] = jnp.where(hit, 1.0, 0.0).astype(jnp.bfloat16)
    late = lax.broadcasted_iota(jnp.int32, year.shape, 1) >= first_sums.shape[1]
    short[0] = 1 - jnp.max(jnp.where(late & (year[...] >= 0), 1, 0))
    for row in range(6):
        fetches[6 + row].wait()
        table[row : row + 1, :] = held[6 + row][...].astype(jnp.float32)


def shard_sums(inputs):
    rows, columns = inputs[0].shape
    count = inputs[6].shape[0]
    views = [
        inputs[0],
        inputs[1].reshape(1, -1),
        inputs[2].reshape(1, -1),
        inputs[3].reshape(1, -1),
        inputs[4].T,
        inputs[5].T,
        *(column.reshape(1, -1) for column in inputs[6:]),
    ]
    views = [pltpu.with_memory_space_constraint(view, pltpu.HBM) for view in views]
    return pl.pallas_call(
        shard_sums_kernel,
        out_shape=(
            jax.ShapeDtypeStruct((TREATIES, rows), jnp.bfloat16),
            jax.ShapeDtypeStruct((TREATIES, rows // 2), jnp.bfloat16),
            jax.ShapeDtypeStruct((8, count), jnp.float32),
            jax.ShapeDtypeStruct((YEAR_DEV, rows), jnp.bfloat16),
            pltpu.SMEM((1,), jnp.int32),
        ),
        in_specs=[HBM] * len(views),
        out_specs=(VMEM, VMEM, VMEM, VMEM, SMEM),
        scratch_shapes=[
            *(pltpu.VMEM(view.shape, view.dtype) for view in views),
            pltpu.VMEM((TREATIES, columns), jnp.bfloat16),
            pltpu.VMEM((rows, columns), jnp.bfloat16),
            pltpu.SemaphoreType.DMA((len(views),)),
        ],
        compiler_params=PARAMS,
        name="shard_sums",
    )(*views)


def as_column(row):
    count = row.shape[1]
    down = lax.broadcasted_iota(jnp.int32, (count, count), 0)
    across = lax.broadcasted_iota(jnp.int32, (count, count), 1)
    return jnp.sum(jnp.where(down == across, row, 0.0), axis=1, keepdims=True)


def in_two(values):
    high = values.astype(jnp.bfloat16)
    low = (values - high.astype(jnp.float32)).astype(jnp.bfloat16)
    return [high, low]


def annual_kernel(blocks, table, hits, annual, kept, sent):
    count = table.shape[1]
    total = blocks[0].astype(jnp.float32)
    for shard in range(1, blocks.shape[0]):
        total = total + blocks[shard].astype(jnp.float32)
    attach = table[0:1, :] * UNIT_LOSS
    limit = table[1:2, :] * UNIT_LOSS
    recovered = clamp_between(total - as_column(attach), 0.0, as_column(limit))
    retained = total - recovered
    pieces = jnp.concatenate(in_two(recovered) + in_two(retained), axis=0)
    yearly = lax.dot_general(
        hits[:, : total.shape[1]], pieces, BY_ROWS, preferred_element_type=jnp.float32
    )
    annual[...] = yearly[:, :count] + yearly[:, count : 2 * count]
    kept_annual = yearly[:, 2 * count : 3 * count] + yearly[:, 3 * count :]
    kept[...] = kept_annual
    half = YEAR_DEV // 2
    line = jnp.concatenate((kept_annual[:half], kept_annual[half:]), axis=1)
    line = line.astype(jnp.bfloat16)
    for peer in range(sent.shape[0]):
        sent[peer] = line


def annual_tables(blocks, table, hits, peers):
    count = table.shape[1]
    tables = jax.ShapeDtypeStruct((YEAR_DEV, count), jnp.float32)
    return pl.pallas_call(
        annual_kernel,
        out_shape=(
            tables,
            tables,
            jax.ShapeDtypeStruct((peers, YEAR_DEV // 2, 2 * count), jnp.bfloat16),
        ),
        in_specs=[VMEM] * 3,
        out_specs=(VMEM, VMEM, VMEM),
        compiler_params=PARAMS,
        name="annual_tables",
    )(blocks, table, hits)


def exchange(items, low, high):
    items[low], items[high] = (
        jnp.maximum(items[low], items[high]),
        jnp.minimum(items[low], items[high]),
    )


def sort_falling(items):
    count = len(items)
    step = 1
    while step < count:
        gap = step
        while gap >= 1:
            for base in range(gap % step, count - gap, 2 * gap):
                for at in range(base, base + min(gap, count - base - gap)):
                    if at // (2 * step) == (at + gap) // (2 * step):
                        exchange(items, at, at + gap)
            gap //= 2
        step *= 2


def larger_half(first, second):
    return [jnp.maximum(one, two) for one, two in zip(first, reversed(second))]


def sort_bitonic(items):
    gap = len(items) // 2
    while gap >= 1:
        for at in range(len(items)):
            if at & gap == 0:
                exchange(items, at, at + gap)
        gap //= 2


def outcome_kernel(everyone, annual, kept, table, net, stop_loss, tail_mean):
    limit = table[1:2, :] * UNIT_LOSS
    again = table[2:3, :]
    rate = table[3:4, :]
    paid = jnp.minimum(annual[...], (1.0 + again) * limit)
    net[...] = (paid - rate * jnp.minimum(paid, again * limit)) / limit
    peers, rows, lanes = everyone.shape
    count = lanes // 2
    tiles = [
        line[at : at + 8, :]
        for line in (everyone[peer].astype(jnp.float32) for peer in range(peers))
        for at in range(0, rows, 8)
    ]
    total = tiles[0]
    for tile in tiles[1:]:
        total = total + tile
    summed = jnp.sum(total, axis=0, keepdims=True)
    summed = summed + pltpu.roll(summed, count, 1)
    base_loss = UNIT_LOSS + summed / (peers * YEAR_DEV)
    largest = None
    for at in range(0, len(tiles), TAIL):
        group = tiles[at : at + TAIL]
        sort_falling(group)
        if largest is None:
            largest = group
        else:
            largest = larger_half(largest, group)
            sort_bitonic(largest)
    for shift in (4, 2, 1):
        largest = larger_half(largest, [pltpu.roll(item, shift, 0) for item in largest])
        sort_bitonic(largest)
    largest = larger_half(largest, [pltpu.roll(item, count, 1) for item in largest])
    top = largest[0]
    for item in largest[1:]:
        top = top + item
    tail_mean[...] = (top[0:1, :] / base_loss / TAIL)[:, :count]
    stop_loss[...] = clamp_between(
        kept[...] / base_loss[:, :count] - table[4:5, :], 0.0, table[5:6, :]
    )


def outcomes(everyone, annual, kept, table):
    return pl.pallas_call(
        outcome_kernel,
        out_shape=(
            jax.ShapeDtypeStruct(kept.shape, jnp.float32),
            jax.ShapeDtypeStruct(kept.shape, jnp.float32),
            jax.ShapeDtypeStruct((1, kept.shape[1]), jnp.float32),
        ),
        in_specs=[VMEM] * 4,
        out_specs=(VMEM, VMEM, VMEM),
        compiler_params=PARAMS,
        name="outcomes",
    )(everyone, annual, kept, table)


def on_device(*inputs):
    ports = lax.axis_size("port")
    years = lax.axis_size("year")
    sums, first_sums, table, hits, short = shard_sums(inputs)

    def exchanged(rows):
        blocks = lax.all_to_all(
            rows.reshape(ports, -1, rows.shape[1]), "port", 0, 0, tiled=True
        )
        return annual_tables(blocks, table, hits, years)

    annual, kept, sent = lax.cond(
        short[0] == 1, lambda: exchanged(first_sums), lambda: exchanged(sums)
    )
    everyone = lax.all_to_all(sent, "year", 0, 0, tiled=True)
    net, stop_loss, tail_mean = outcomes(everyone, annual, kept, table)
    return (net.T, stop_loss.T, tail_mean.reshape(-1))


def solution(mesh):
    return jax.shard_map(
        on_device,
        mesh=mesh,
        in_specs=(
            P("year", "port"),
            P("year"),
            P("port"),
            P("port"),
            P("port", None),
            P("port", None),
            P("port"),
            P("port"),
            P("port"),
            P("port"),
            P("port"),
            P("port"),
        ),
        out_specs=(P("port", "year"), P("port", "year"), P("port")),
        check_vma=False,
    )
```

```python
import jax
import jax.numpy as jnp
from jax import lax
from jax.experimental import pallas as pl
from jax.experimental.pallas import tpu as pltpu
from jax.sharding import PartitionSpec as P

TREATIES = 1024
MEMB = 4
YEAR_DEV = 32
TAIL = 16
LANES = 128
BLOCK = 256

UNIT_LOSS = 1.0

VMEM = pl.BlockSpec(memory_space=pltpu.VMEM)
SMEM = pl.BlockSpec(memory_space=pltpu.SMEM)
HBM = pl.BlockSpec(memory_space=pltpu.HBM)
PARAMS = pltpu.CompilerParams(vmem_limit_bytes=16 * 1024 * 1024)
BY_ROWS = (((1,), (1,)), ((), ()))


def clamp_between(values, lower, upper):
    return jnp.minimum(jnp.maximum(values, lower), upper)


def shard_sums_kernel(*refs):
    inputs, outputs, held = refs[:12], refs[12:17], refs[17:29]
    sums, first_sums, table, hits, short = outputs
    weights, ceded, arrived = refs[29:]
    order = (5, 4, 2, 3, 0, 1, 6, 7, 8, 9, 10, 11)
    fetches = {
        k: pltpu.make_async_copy(inputs[k], held[k], arrived.at[k]) for k in order
    }
    for k in order:
        fetches[k].start()
    loss, year, retention, risk_limit, share, member = held[:6]
    columns = loss.shape[1]
    treaty = lax.broadcasted_iota(jnp.int32, (BLOCK, LANES), 0)
    treaty = treaty.astype(jnp.float32).astype(jnp.bfloat16)
    zero = jnp.zeros((BLOCK, LANES), jnp.bfloat16)
    fetches[5].wait()
    fetches[4].wait()
    named = member[...]
    part = share[...]

    def build(first):
        local = named - first
        inside = (local >= 0) & (local < BLOCK)
        local = jnp.where(inside, local, BLOCK).astype(jnp.float32).astype(jnp.bfloat16)
        for at in range(0, columns, LANES):
            block = zero
            for slot in range(MEMB):
                hit = treaty == local[slot : slot + 1, at : at + LANES]
                block = jnp.where(hit, part[slot : slot + 1, at : at + LANES], block)
            weights[first : first + BLOCK, at : at + LANES] = block

    def multiply(first):
        block = lax.dot_general(
            weights[first : first + BLOCK, :],
            ceded[...],
            BY_ROWS,
            preferred_element_type=jnp.float32,
        ).astype(jnp.bfloat16)
        sums[first : first + BLOCK, :] = block
        first_sums[first : first + BLOCK, :] = block[:, : first_sums.shape[1]]

    blocks = list(range(0, TREATIES, BLOCK))
    ahead = 2
    for first in blocks[:ahead]:
        build(first)
    fetches[2].wait()
    fetches[3].wait()
    fetches[0].wait()
    ceded[...] = clamp_between(
        loss[...].astype(jnp.float32) - retention[...], 0.0, risk_limit[...]
    ).astype(jnp.bfloat16)
    for k, first in enumerate(blocks):
        multiply(first)
        if k + ahead < len(blocks):
            build(blocks[k + ahead])
    fetches[1].wait()
    local_year = jnp.where(year[...] < 0, -1, year[...] & (YEAR_DEV - 1))
    hit = lax.broadcasted_iota(jnp.int32, hits.shape, 0) == local_year
    hits[...] = jnp.where(hit, 1.0, 0.0).astype(jnp.bfloat16)
    late = lax.broadcasted_iota(jnp.int32, year.shape, 1) >= first_sums.shape[1]
    short[0] = 1 - jnp.max(jnp.where(late & (year[...] >= 0), 1, 0))
    for row in range(6):
        fetches[6 + row].wait()
        table[row : row + 1, :] = held[6 + row][...].astype(jnp.float32)


def shard_sums(inputs):
    rows, columns = inputs[0].shape
    count = inputs[6].shape[0]
    views = [
        inputs[0],
        inputs[1].reshape(1, -1),
        inputs[2].reshape(1, -1),
        inputs[3].reshape(1, -1),
        inputs[4].T,
        inputs[5].T,
        *(column.reshape(1, -1) for column in inputs[6:]),
    ]
    views = [pltpu.with_memory_space_constraint(view, pltpu.HBM) for view in views]
    return pl.pallas_call(
        shard_sums_kernel,
        out_shape=(
            jax.ShapeDtypeStruct((TREATIES, rows), jnp.bfloat16),
            jax.ShapeDtypeStruct((TREATIES, rows // 2), jnp.bfloat16),
            jax.ShapeDtypeStruct((8, count), jnp.float32),
            jax.ShapeDtypeStruct((YEAR_DEV, rows), jnp.bfloat16),
            pltpu.SMEM((1,), jnp.int32),
        ),
        in_specs=[HBM] * len(views),
        out_specs=(VMEM, VMEM, VMEM, VMEM, SMEM),
        scratch_shapes=[
            *(pltpu.VMEM(view.shape, view.dtype) for view in views),
            pltpu.VMEM((TREATIES, columns), jnp.bfloat16),
            pltpu.VMEM((rows, columns), jnp.bfloat16),
            pltpu.SemaphoreType.DMA((len(views),)),
        ],
        compiler_params=PARAMS,
        name="shard_sums",
    )(*views)


def as_column(row):
    count = row.shape[1]
    down = lax.broadcasted_iota(jnp.int32, (count, count), 0)
    across = lax.broadcasted_iota(jnp.int32, (count, count), 1)
    return jnp.sum(jnp.where(down == across, row, 0.0), axis=1, keepdims=True)


def in_two(values):
    high = values.astype(jnp.bfloat16)
    low = (values - high.astype(jnp.float32)).astype(jnp.bfloat16)
    return [high, low]


def exchange(items, low, high):
    items[low], items[high] = (
        jnp.maximum(items[low], items[high]),
        jnp.minimum(items[low], items[high]),
    )


def sort_falling(items):
    count = len(items)
    step = 1
    while step < count:
        gap = step
        while gap >= 1:
            for base in range(gap % step, count - gap, 2 * gap):
                for at in range(base, base + min(gap, count - base - gap)):
                    if at // (2 * step) == (at + gap) // (2 * step):
                        exchange(items, at, at + gap)
            gap //= 2
        step *= 2


def larger_half(first, second):
    return [jnp.maximum(one, two) for one, two in zip(first, reversed(second))]


def sort_bitonic(items):
    gap = len(items) // 2
    while gap >= 1:
        for at in range(len(items)):
            if at & gap == 0:
                exchange(items, at, at + gap)
        gap //= 2


def annual_kernel(blocks, table, hits, annual, kept, sent):
    count = table.shape[1]
    total = blocks[0].astype(jnp.float32)
    for shard in range(1, blocks.shape[0]):
        total = total + blocks[shard].astype(jnp.float32)
    attach = table[0:1, :] * UNIT_LOSS
    limit = table[1:2, :] * UNIT_LOSS
    recovered = clamp_between(total - as_column(attach), 0.0, as_column(limit))
    retained = total - recovered
    pieces = jnp.concatenate(in_two(recovered) + in_two(retained), axis=0)
    yearly = lax.dot_general(
        hits[:, : total.shape[1]], pieces, BY_ROWS, preferred_element_type=jnp.float32
    )
    annual[...] = yearly[:, :count] + yearly[:, count : 2 * count]
    kept_annual = yearly[:, 2 * count : 3 * count] + yearly[:, 3 * count :]
    kept[...] = kept_annual
    line = jnp.concatenate((kept_annual[:TAIL], kept_annual[TAIL:]), axis=1)
    years = [jnp.broadcast_to(line[k : k + 1], (8, 2 * count)) for k in range(TAIL)]
    sort_falling(years)
    years = larger_half(years, [pltpu.roll(item, count, 1) for item in years])[: TAIL // 2]
    summed = jnp.sum(kept_annual, axis=0, keepdims=True)
    high, low = [part.astype(jnp.float32) for part in in_two(summed)]
    sums = jnp.broadcast_to(jnp.concatenate((high, low), axis=1), (8, 2 * count))
    rows = years + [sums] * 4
    down = lax.broadcasted_iota(jnp.int32, (8, 2 * count), 0)
    for chunk in range(3):
        packed = rows[4 * chunk + 3]
        for k in range(3):
            packed = jnp.where(down == k, rows[4 * chunk + k], packed)
        packed = packed[:4].astype(jnp.bfloat16)
        for peer in range(sent.shape[0]):
            sent[peer, :, 2 * count * chunk : 2 * count * (chunk + 1)] = packed


def annual_tables(blocks, table, hits, peers):
    count = table.shape[1]
    tables = jax.ShapeDtypeStruct((YEAR_DEV, count), jnp.float32)
    return pl.pallas_call(
        annual_kernel,
        out_shape=(
            tables,
            tables,
            jax.ShapeDtypeStruct((peers, 4, 6 * count), jnp.bfloat16),
        ),
        in_specs=[VMEM] * 3,
        out_specs=(VMEM, VMEM, VMEM),
        compiler_params=PARAMS,
        name="annual_tables",
    )(blocks, table, hits)


def outcome_kernel(everyone, annual, kept, table, net, stop_loss, tail_mean):
    limit = table[1:2, :] * UNIT_LOSS
    again = table[2:3, :]
    rate = table[3:4, :]
    paid = jnp.minimum(annual[...], (1.0 + again) * limit)
    net[...] = (paid - rate * jnp.minimum(paid, again * limit)) / limit
    peers = everyone.shape[0]
    count = everyone.shape[2] // 6
    lanes = 2 * count

    def chunk(peer, at, rows):
        return everyone[peer, :rows, at * lanes : (at + 1) * lanes].astype(jnp.float32)

    tiles = [
        jnp.concatenate((chunk(peer, at, 4), chunk(peer + 1, at, 4)), axis=0)
        for peer in range(0, peers, 2)
        for at in range(2)
    ]
    summed = chunk(0, 2, 4)
    for peer in range(1, peers):
        summed = summed + chunk(peer, 2, 4)
    summed = summed[:1]
    summed = summed + pltpu.roll(summed, count, 1)
    base_loss = UNIT_LOSS + summed / (peers * YEAR_DEV)
    largest = None
    for at in range(0, len(tiles), TAIL):
        group = tiles[at : at + TAIL]
        sort_falling(group)
        if largest is None:
            largest = group
        else:
            largest = larger_half(largest, group)
            sort_bitonic(largest)
    for shift in (4, 2, 1):
        largest = larger_half(largest, [pltpu.roll(item, shift, 0) for item in largest])
        sort_bitonic(largest)
    largest = larger_half(largest, [pltpu.roll(item, count, 1) for item in largest])
    top = largest[0]
    for item in largest[1:]:
        top = top + item
    tail_mean[...] = (top[0:1, :] / base_loss / TAIL)[:, :count]
    stop_loss[...] = clamp_between(
        kept[...] / base_loss[:, :count] - table[4:5, :], 0.0, table[5:6, :]
    )


def outcomes(everyone, annual, kept, table):
    return pl.pallas_call(
        outcome_kernel,
        out_shape=(
            jax.ShapeDtypeStruct(kept.shape, jnp.float32),
            jax.ShapeDtypeStruct(kept.shape, jnp.float32),
            jax.ShapeDtypeStruct((1, kept.shape[1]), jnp.float32),
        ),
        in_specs=[VMEM] * 4,
        out_specs=(VMEM, VMEM, VMEM),
        compiler_params=PARAMS,
        name="outcomes",
    )(everyone, annual, kept, table)


def on_device(*inputs):
    ports = lax.axis_size("port")
    years = lax.axis_size("year")
    sums, first_sums, table, hits, short = shard_sums(inputs)

    def exchanged(rows):
        blocks = lax.all_to_all(
            rows.reshape(ports, -1, rows.shape[1]), "port", 0, 0, tiled=True
        )
        return annual_tables(blocks, table, hits, years)

    annual, kept, sent = lax.cond(
        short[0] == 1, lambda: exchanged(first_sums), lambda: exchanged(sums)
    )
    everyone = lax.all_to_all(sent, "year", 0, 0, tiled=True)
    net, stop_loss, tail_mean = outcomes(everyone, annual, kept, table)
    return (net.T, stop_loss.T, tail_mean.reshape(-1))


def solution(mesh):
    return jax.shard_map(
        on_device,
        mesh=mesh,
        in_specs=(
            P("year", "port"),
            P("year"),
            P("port"),
            P("port"),
            P("port", None),
            P("port", None),
            P("port"),
            P("port"),
            P("port"),
            P("port"),
            P("port"),
            P("port"),
        ),
        out_specs=(P("port", "year"), P("port", "year"), P("port")),
        check_vma=False,
    )
```

```python
import functools

import jax
import jax.numpy as jnp
from jax import lax
from jax.experimental import pallas as pl
from jax.experimental.pallas import tpu as pltpu
from jax.sharding import PartitionSpec as P

TREATIES = 1024
MEMB = 4
YEAR_DEV = 32
TAIL = 16
LANES = 128
BLOCK = 256

UNIT_LOSS = 1.0

VMEM = pl.BlockSpec(memory_space=pltpu.VMEM)
SMEM = pl.BlockSpec(memory_space=pltpu.SMEM)
HBM = pl.BlockSpec(memory_space=pltpu.HBM)
PARAMS = pltpu.CompilerParams(vmem_limit_bytes=16 * 1024 * 1024)
BY_ROWS = (((1,), (1,)), ((), ()))


def clamp_between(values, lower, upper):
    return jnp.minimum(jnp.maximum(values, lower), upper)


def shard_sums_kernel(*refs):
    inputs, outputs, held = refs[:12], refs[12:16], refs[16:28]
    sums, table, hits, strips = outputs
    weights, ceded, arrived = refs[28:]
    count = table.shape[1]
    order = (5, 4, 2, 3, 0, 1, 6, 7, 8, 9, 10, 11)
    fetches = {
        k: pltpu.make_async_copy(inputs[k], held[k], arrived.at[k]) for k in order
    }
    for k in order:
        fetches[k].start()
    loss, year, retention, risk_limit, share, member = held[:6]
    columns = loss.shape[1]
    treaty = lax.broadcasted_iota(jnp.int32, (BLOCK, LANES), 0)
    treaty = treaty.astype(jnp.float32).astype(jnp.bfloat16)
    zero = jnp.zeros((BLOCK, LANES), jnp.bfloat16)
    fetches[5].wait()
    fetches[4].wait()
    named = member[...]
    part = share[...]

    def build(first):
        local = named - first
        inside = (local >= 0) & (local < BLOCK)
        local = jnp.where(inside, local, BLOCK).astype(jnp.float32).astype(jnp.bfloat16)
        for at in range(0, columns, LANES):
            block = zero
            for slot in range(MEMB):
                hit = treaty == local[slot : slot + 1, at : at + LANES]
                block = jnp.where(hit, part[slot : slot + 1, at : at + LANES], block)
            weights[first : first + BLOCK, at : at + LANES] = block

    def multiply(first):
        block = lax.dot_general(
            weights[first : first + BLOCK, :],
            ceded[...],
            BY_ROWS,
            preferred_element_type=jnp.float32,
        ).astype(jnp.bfloat16)
        for owner in range(BLOCK // count):
            for strip in range(block.shape[1] // LANES):
                sums[first // count + owner, strip * count : (strip + 1) * count, :] = block[
                    owner * count : (owner + 1) * count, strip * LANES : (strip + 1) * LANES
                ]

    blocks = list(range(0, TREATIES, BLOCK))
    ahead = 2
    for first in blocks[:ahead]:
        build(first)
    fetches[1].wait()
    local_year = jnp.where(year[...] < 0, -1, year[...] & (YEAR_DEV - 1))
    hit = lax.broadcasted_iota(jnp.int32, hits.shape, 0) == local_year
    hits[...] = jnp.where(hit, 1.0, 0.0).astype(jnp.bfloat16)
    strip = lax.broadcasted_iota(jnp.int32, year.shape, 1) // LANES
    strips[0] = jnp.max(jnp.where(year[...] >= 0, strip, 0))
    for row in range(6):
        fetches[6 + row].wait()
        table[row : row + 1, :] = held[6 + row][...].astype(jnp.float32)
    fetches[2].wait()
    fetches[3].wait()
    fetches[0].wait()
    ceded[...] = clamp_between(
        loss[...].astype(jnp.float32) - retention[...], 0.0, risk_limit[...]
    ).astype(jnp.bfloat16)
    for k, first in enumerate(blocks):
        multiply(first)
        if k + ahead < len(blocks):
            build(blocks[k + ahead])


def shard_sums(inputs):
    rows, columns = inputs[0].shape
    count = inputs[6].shape[0]
    views = [
        inputs[0],
        inputs[1].reshape(1, -1),
        inputs[2].reshape(1, -1),
        inputs[3].reshape(1, -1),
        inputs[4].T,
        inputs[5].T,
        *(column.reshape(1, -1) for column in inputs[6:]),
    ]
    views = [pltpu.with_memory_space_constraint(view, pltpu.HBM) for view in views]
    return pl.pallas_call(
        shard_sums_kernel,
        out_shape=(
            jax.ShapeDtypeStruct((TREATIES // count, rows // LANES * count, LANES), jnp.bfloat16),
            jax.ShapeDtypeStruct((8, count), jnp.float32),
            jax.ShapeDtypeStruct((YEAR_DEV, rows), jnp.bfloat16),
            pltpu.SMEM((1,), jnp.int32),
        ),
        in_specs=[HBM] * len(views),
        out_specs=(VMEM, VMEM, VMEM, SMEM),
        scratch_shapes=[
            *(pltpu.VMEM(view.shape, view.dtype) for view in views),
            pltpu.VMEM((TREATIES, columns), jnp.bfloat16),
            pltpu.VMEM((rows, columns), jnp.bfloat16),
            pltpu.SemaphoreType.DMA((len(views),)),
        ],
        compiler_params=PARAMS,
        name="shard_sums",
    )(*views)


def as_column(row):
    count = row.shape[1]
    down = lax.broadcasted_iota(jnp.int32, (count, count), 0)
    across = lax.broadcasted_iota(jnp.int32, (count, count), 1)
    return jnp.sum(jnp.where(down == across, row, 0.0), axis=1, keepdims=True)


def in_two(values):
    high = values.astype(jnp.bfloat16)
    low = (values - high.astype(jnp.float32)).astype(jnp.bfloat16)
    return [high, low]


def exchange(items, low, high):
    items[low], items[high] = (
        jnp.maximum(items[low], items[high]),
        jnp.minimum(items[low], items[high]),
    )


def sort_falling(items):
    count = len(items)
    step = 1
    while step < count:
        gap = step
        while gap >= 1:
            for base in range(gap % step, count - gap, 2 * gap):
                for at in range(base, base + min(gap, count - base - gap)):
                    if at // (2 * step) == (at + gap) // (2 * step):
                        exchange(items, at, at + gap)
            gap //= 2
        step *= 2


def larger_half(first, second):
    return [jnp.maximum(one, two) for one, two in zip(first, reversed(second))]


def sort_bitonic(items):
    gap = len(items) // 2
    while gap >= 1:
        for at in range(len(items)):
            if at & gap == 0:
                exchange(items, at, at + gap)
        gap //= 2


def annual_kernel(blocks, table, hits, annual, kept, sent):
    count = table.shape[1]
    parts = []
    for at in range(0, blocks.shape[1], count):
        part = blocks[0, at : at + count, :].astype(jnp.float32)
        for shard in range(1, blocks.shape[0]):
            part = part + blocks[shard, at : at + count, :].astype(jnp.float32)
        parts.append(part)
    total = jnp.concatenate(parts, axis=1)
    attach = table[0:1, :] * UNIT_LOSS
    limit = table[1:2, :] * UNIT_LOSS
    recovered = clamp_between(total - as_column(attach), 0.0, as_column(limit))
    retained = total - recovered
    pieces = jnp.concatenate(in_two(recovered) + in_two(retained), axis=0)
    yearly = lax.dot_general(
        hits[:, : total.shape[1]], pieces, BY_ROWS, preferred_element_type=jnp.float32
    )
    annual[...] = yearly[:, :count] + yearly[:, count : 2 * count]
    kept_annual = yearly[:, 2 * count : 3 * count] + yearly[:, 3 * count :]
    kept[...] = kept_annual
    line = jnp.concatenate((kept_annual[:TAIL], kept_annual[TAIL:]), axis=1)
    years = [jnp.broadcast_to(line[k : k + 1], (8, 2 * count)) for k in range(TAIL)]
    sort_falling(years)
    years = larger_half(years, [pltpu.roll(item, count, 1) for item in years])[: TAIL // 2]
    summed = jnp.sum(kept_annual, axis=0, keepdims=True)
    high, low = [part.astype(jnp.float32) for part in in_two(summed)]
    sums = jnp.broadcast_to(jnp.concatenate((high, low), axis=1), (8, 2 * count))
    rows = years + [sums] * 4
    down = lax.broadcasted_iota(jnp.int32, (8, 2 * count), 0)
    for chunk in range(3):
        packed = rows[4 * chunk + 3]
        for k in range(3):
            packed = jnp.where(down == k, rows[4 * chunk + k], packed)
        packed = packed[:4].astype(jnp.bfloat16)
        for peer in range(sent.shape[0]):
            sent[peer, :, 2 * count * chunk : 2 * count * (chunk + 1)] = packed


def annual_tables(blocks, table, hits, peers):
    count = table.shape[1]
    tables = jax.ShapeDtypeStruct((YEAR_DEV, count), jnp.float32)
    return pl.pallas_call(
        annual_kernel,
        out_shape=(
            tables,
            tables,
            jax.ShapeDtypeStruct((peers, 4, 6 * count), jnp.bfloat16),
        ),
        in_specs=[VMEM] * 3,
        out_specs=(VMEM, VMEM, VMEM),
        compiler_params=PARAMS,
        name="annual_tables",
    )(blocks, table, hits)


def outcome_kernel(everyone, annual, kept, table, net, stop_loss, tail_mean):
    limit = table[1:2, :] * UNIT_LOSS
    again = table[2:3, :]
    rate = table[3:4, :]
    paid = jnp.minimum(annual[...], (1.0 + again) * limit)
    net[...] = (paid - rate * jnp.minimum(paid, again * limit)) / limit
    peers = everyone.shape[0]
    count = everyone.shape[2] // 6
    lanes = 2 * count

    def chunk(peer, at, rows):
        return everyone[peer, :rows, at * lanes : (at + 1) * lanes].astype(jnp.float32)

    tiles = [
        jnp.concatenate((chunk(peer, at, 4), chunk(peer + 1, at, 4)), axis=0)
        for peer in range(0, peers, 2)
        for at in range(2)
    ]
    summed = chunk(0, 2, 4)
    for peer in range(1, peers):
        summed = summed + chunk(peer, 2, 4)
    summed = summed[:1]
    summed = summed + pltpu.roll(summed, count, 1)
    base_loss = UNIT_LOSS + summed / (peers * YEAR_DEV)
    largest = None
    for at in range(0, len(tiles), TAIL):
        group = tiles[at : at + TAIL]
        sort_falling(group)
        if largest is None:
            largest = group
        else:
            largest = larger_half(largest, group)
            sort_bitonic(largest)
    for shift in (4, 2, 1):
        largest = larger_half(largest, [pltpu.roll(item, shift, 0) for item in largest])
        sort_bitonic(largest)
    largest = larger_half(largest, [pltpu.roll(item, count, 1) for item in largest])
    top = largest[0]
    for item in largest[1:]:
        top = top + item
    tail_mean[...] = (top[0:1, :] / base_loss / TAIL)[:, :count]
    stop_loss[...] = clamp_between(
        kept[...] / base_loss[:, :count] - table[4:5, :], 0.0, table[5:6, :]
    )


def outcomes(everyone, annual, kept, table):
    return pl.pallas_call(
        outcome_kernel,
        out_shape=(
            jax.ShapeDtypeStruct(kept.shape, jnp.float32),
            jax.ShapeDtypeStruct(kept.shape, jnp.float32),
            jax.ShapeDtypeStruct((1, kept.shape[1]), jnp.float32),
        ),
        in_specs=[VMEM] * 4,
        out_specs=(VMEM, VMEM, VMEM),
        compiler_params=PARAMS,
        name="outcomes",
    )(everyone, annual, kept, table)


def on_device(*inputs):
    years = lax.axis_size("year")
    sums, table, hits, strips = shard_sums(inputs)
    count = table.shape[1]

    def exchanged(taken):
        rows = sums[:, : taken * count, :]
        blocks = lax.all_to_all(rows, "port", 0, 0, tiled=True)
        return annual_tables(blocks, table, hits, years)

    branches = [
        functools.partial(exchanged, taken + 1) for taken in range(sums.shape[1] // count)
    ]
    annual, kept, sent = lax.switch(strips[0], branches)
    everyone = lax.all_to_all(sent, "year", 0, 0, tiled=True)
    net, stop_loss, tail_mean = outcomes(everyone, annual, kept, table)
    return (net.T, stop_loss.T, tail_mean.reshape(-1))


def solution(mesh):
    return jax.shard_map(
        on_device,
        mesh=mesh,
        in_specs=(
            P("year", "port"),
            P("year"),
            P("port"),
            P("port"),
            P("port", None),
            P("port", None),
            P("port"),
            P("port"),
            P("port"),
            P("port"),
            P("port"),
            P("port"),
        ),
        out_specs=(P("port", "year"), P("port", "year"), P("port")),
        check_vma=False,
    )
```

```python
import functools

import jax
import jax.numpy as jnp
from jax import lax
from jax.experimental import pallas as pl
from jax.experimental.pallas import tpu as pltpu
from jax.sharding import Mesh, PartitionSpec as P

TREATIES = 1024
MEMB = 4
YEAR_DEV = 32
TAIL = 16
LANES = 128
BLOCK = 256
NEAR = ("z_pair", "x_pair")
SQUARE = 4
FAR = "z_far"

UNIT_LOSS = 1.0

VMEM = pl.BlockSpec(memory_space=pltpu.VMEM)
SMEM = pl.BlockSpec(memory_space=pltpu.SMEM)
HBM = pl.BlockSpec(memory_space=pltpu.HBM)
PARAMS = pltpu.CompilerParams(vmem_limit_bytes=16 * 1024 * 1024)
BY_ROWS = (((1,), (1,)), ((), ()))


def clamp_between(values, lower, upper):
    return jnp.minimum(jnp.maximum(values, lower), upper)


def shard_sums_kernel(*refs):
    inputs, outputs, held = refs[:12], refs[12:16], refs[16:28]
    sums, table, hits, strips = outputs
    weights, ceded, arrived = refs[28:]
    count = table.shape[1]
    order = (5, 4, 2, 3, 0, 1, 6, 7, 8, 9, 10, 11)
    fetches = {
        k: pltpu.make_async_copy(inputs[k], held[k], arrived.at[k]) for k in order
    }
    for k in order:
        fetches[k].start()
    loss, year, retention, risk_limit, share, member = held[:6]
    columns = loss.shape[1]
    treaty = lax.broadcasted_iota(jnp.int32, (BLOCK, LANES), 0)
    treaty = treaty.astype(jnp.float32).astype(jnp.bfloat16)
    zero = jnp.zeros((BLOCK, LANES), jnp.bfloat16)
    fetches[5].wait()
    fetches[4].wait()
    named = member[...]
    part = share[...]

    def build(first):
        local = named - first
        inside = (local >= 0) & (local < BLOCK)
        local = jnp.where(inside, local, BLOCK).astype(jnp.float32).astype(jnp.bfloat16)
        for at in range(0, columns, LANES):
            block = zero
            for slot in range(MEMB):
                hit = treaty == local[slot : slot + 1, at : at + LANES]
                block = jnp.where(hit, part[slot : slot + 1, at : at + LANES], block)
            weights[first : first + BLOCK, at : at + LANES] = block

    def multiply(first):
        block = lax.dot_general(
            weights[first : first + BLOCK, :],
            ceded[...],
            BY_ROWS,
            preferred_element_type=jnp.float32,
        ).astype(jnp.bfloat16)
        for at in range(BLOCK // count):
            owner = first // count + at
            slot = owner % SQUARE * (sums.shape[0] // SQUARE) + owner // SQUARE
            for strip in range(block.shape[1] // LANES):
                sums[slot, strip * count : (strip + 1) * count, :] = block[
                    at * count : (at + 1) * count, strip * LANES : (strip + 1) * LANES
                ]

    blocks = list(range(0, TREATIES, BLOCK))
    ahead = 2
    for first in blocks[:ahead]:
        build(first)
    fetches[1].wait()
    local_year = jnp.where(year[...] < 0, -1, year[...] & (YEAR_DEV - 1))
    hit = lax.broadcasted_iota(jnp.int32, hits.shape, 0) == local_year
    hits[...] = jnp.where(hit, 1.0, 0.0).astype(jnp.bfloat16)
    strip = lax.broadcasted_iota(jnp.int32, year.shape, 1) // LANES
    strips[0] = jnp.max(jnp.where(year[...] >= 0, strip, 0))
    for row in range(6):
        fetches[6 + row].wait()
        table[row : row + 1, :] = held[6 + row][...].astype(jnp.float32)
    fetches[2].wait()
    fetches[3].wait()
    fetches[0].wait()
    ceded[...] = clamp_between(
        loss[...].astype(jnp.float32) - retention[...], 0.0, risk_limit[...]
    ).astype(jnp.bfloat16)
    for k, first in enumerate(blocks):
        multiply(first)
        if k + ahead < len(blocks):
            build(blocks[k + ahead])


def shard_sums(inputs):
    rows, columns = inputs[0].shape
    count = inputs[6].shape[0]
    views = [
        inputs[0],
        inputs[1].reshape(1, -1),
        inputs[2].reshape(1, -1),
        inputs[3].reshape(1, -1),
        inputs[4].T,
        inputs[5].T,
        *(column.reshape(1, -1) for column in inputs[6:]),
    ]
    views = [pltpu.with_memory_space_constraint(view, pltpu.HBM) for view in views]
    return pl.pallas_call(
        shard_sums_kernel,
        out_shape=(
            jax.ShapeDtypeStruct((TREATIES // count, rows // LANES * count, LANES), jnp.bfloat16),
            jax.ShapeDtypeStruct((8, count), jnp.float32),
            jax.ShapeDtypeStruct((YEAR_DEV, rows), jnp.bfloat16),
            pltpu.SMEM((1,), jnp.int32),
        ),
        in_specs=[HBM] * len(views),
        out_specs=(VMEM, VMEM, VMEM, SMEM),
        scratch_shapes=[
            *(pltpu.VMEM(view.shape, view.dtype) for view in views),
            pltpu.VMEM((TREATIES, columns), jnp.bfloat16),
            pltpu.VMEM((rows, columns), jnp.bfloat16),
            pltpu.SemaphoreType.DMA((len(views),)),
        ],
        compiler_params=PARAMS,
        name="shard_sums",
    )(*views)


def as_column(row):
    count = row.shape[1]
    down = lax.broadcasted_iota(jnp.int32, (count, count), 0)
    across = lax.broadcasted_iota(jnp.int32, (count, count), 1)
    return jnp.sum(jnp.where(down == across, row, 0.0), axis=1, keepdims=True)


def in_two(values):
    high = values.astype(jnp.bfloat16)
    low = (values - high.astype(jnp.float32)).astype(jnp.bfloat16)
    return [high, low]


def exchange(items, low, high):
    items[low], items[high] = (
        jnp.maximum(items[low], items[high]),
        jnp.minimum(items[low], items[high]),
    )


def sort_falling(items):
    count = len(items)
    step = 1
    while step < count:
        gap = step
        while gap >= 1:
            for base in range(gap % step, count - gap, 2 * gap):
                for at in range(base, base + min(gap, count - base - gap)):
                    if at // (2 * step) == (at + gap) // (2 * step):
                        exchange(items, at, at + gap)
            gap //= 2
        step *= 2


def larger_half(first, second):
    return [jnp.maximum(one, two) for one, two in zip(first, reversed(second))]


def sort_bitonic(items):
    gap = len(items) // 2
    while gap >= 1:
        for at in range(len(items)):
            if at & gap == 0:
                exchange(items, at, at + gap)
        gap //= 2


def annual_kernel(blocks, table, hits, annual, kept, sent):
    count = table.shape[1]
    parts = []
    for at in range(0, blocks.shape[1], count):
        part = blocks[0, at : at + count, :].astype(jnp.float32)
        for shard in range(1, blocks.shape[0]):
            part = part + blocks[shard, at : at + count, :].astype(jnp.float32)
        parts.append(part)
    total = jnp.concatenate(parts, axis=1)
    attach = table[0:1, :] * UNIT_LOSS
    limit = table[1:2, :] * UNIT_LOSS
    recovered = clamp_between(total - as_column(attach), 0.0, as_column(limit))
    retained = total - recovered
    pieces = jnp.concatenate(in_two(recovered) + in_two(retained), axis=0)
    yearly = lax.dot_general(
        hits[:, : total.shape[1]], pieces, BY_ROWS, preferred_element_type=jnp.float32
    )
    annual[...] = yearly[:, :count] + yearly[:, count : 2 * count]
    kept_annual = yearly[:, 2 * count : 3 * count] + yearly[:, 3 * count :]
    kept[...] = kept_annual
    line = jnp.concatenate((kept_annual[:TAIL], kept_annual[TAIL:]), axis=1)
    years = [jnp.broadcast_to(line[k : k + 1], (8, 2 * count)) for k in range(TAIL)]
    sort_falling(years)
    years = larger_half(years, [pltpu.roll(item, count, 1) for item in years])[: TAIL // 2]
    summed = jnp.sum(kept_annual, axis=0, keepdims=True)
    high, low = [part.astype(jnp.float32) for part in in_two(summed)]
    sums = jnp.broadcast_to(jnp.concatenate((high, low), axis=1), (8, 2 * count))
    rows = years + [sums] * 4
    down = lax.broadcasted_iota(jnp.int32, (8, 2 * count), 0)
    for chunk in range(3):
        packed = rows[4 * chunk + 3]
        for k in range(3):
            packed = jnp.where(down == k, rows[4 * chunk + k], packed)
        packed = packed[:4].astype(jnp.bfloat16)
        for peer in range(sent.shape[0]):
            sent[peer, :, 2 * count * chunk : 2 * count * (chunk + 1)] = packed


def annual_tables(blocks, table, hits, peers):
    count = table.shape[1]
    tables = jax.ShapeDtypeStruct((YEAR_DEV, count), jnp.float32)
    return pl.pallas_call(
        annual_kernel,
        out_shape=(
            tables,
            tables,
            jax.ShapeDtypeStruct((peers, 4, 6 * count), jnp.bfloat16),
        ),
        in_specs=[VMEM] * 3,
        out_specs=(VMEM, VMEM, VMEM),
        compiler_params=PARAMS,
        name="annual_tables",
    )(blocks, table, hits)


def outcome_kernel(everyone, annual, kept, table, net, stop_loss, tail_mean):
    limit = table[1:2, :] * UNIT_LOSS
    again = table[2:3, :]
    rate = table[3:4, :]
    paid = jnp.minimum(annual[...], (1.0 + again) * limit)
    net[...] = (paid - rate * jnp.minimum(paid, again * limit)) / limit
    peers = everyone.shape[0]
    count = everyone.shape[2] // 6
    lanes = 2 * count

    def chunk(peer, at, rows):
        return everyone[peer, :rows, at * lanes : (at + 1) * lanes].astype(jnp.float32)

    tiles = [
        jnp.concatenate((chunk(peer, at, 4), chunk(peer + 1, at, 4)), axis=0)
        for peer in range(0, peers, 2)
        for at in range(2)
    ]
    summed = chunk(0, 2, 4)
    for peer in range(1, peers):
        summed = summed + chunk(peer, 2, 4)
    summed = summed[:1]
    summed = summed + pltpu.roll(summed, count, 1)
    base_loss = UNIT_LOSS + summed / (peers * YEAR_DEV)
    largest = None
    for at in range(0, len(tiles), TAIL):
        group = tiles[at : at + TAIL]
        sort_falling(group)
        if largest is None:
            largest = group
        else:
            largest = larger_half(largest, group)
            sort_bitonic(largest)
    for shift in (4, 2, 1):
        largest = larger_half(largest, [pltpu.roll(item, shift, 0) for item in largest])
        sort_bitonic(largest)
    largest = larger_half(largest, [pltpu.roll(item, count, 1) for item in largest])
    top = largest[0]
    for item in largest[1:]:
        top = top + item
    tail_mean[...] = (top[0:1, :] / base_loss / TAIL)[:, :count]
    stop_loss[...] = clamp_between(
        kept[...] / base_loss[:, :count] - table[4:5, :], 0.0, table[5:6, :]
    )


def outcomes(everyone, annual, kept, table):
    return pl.pallas_call(
        outcome_kernel,
        out_shape=(
            jax.ShapeDtypeStruct(kept.shape, jnp.float32),
            jax.ShapeDtypeStruct(kept.shape, jnp.float32),
            jax.ShapeDtypeStruct((1, kept.shape[1]), jnp.float32),
        ),
        in_specs=[VMEM] * 4,
        out_specs=(VMEM, VMEM, VMEM),
        compiler_params=PARAMS,
        name="outcomes",
    )(everyone, annual, kept, table)


def on_device(*inputs):
    years = lax.axis_size("year")
    sums, table, hits, strips = shard_sums(inputs)
    count = table.shape[1]

    def exchanged(taken):
        rows = sums[:, : taken * count, :]
        blocks = lax.all_to_all(rows, (*NEAR, FAR), 0, 0, tiled=True)
        return annual_tables(blocks, table, hits, years)

    def exchanged_twice():
        rows = sums.reshape(SQUARE, -1, *sums.shape[1:])
        near = lax.all_to_all(rows, NEAR, 0, 0, tiled=True)
        near = jnp.sum(near.astype(jnp.float32), axis=0).astype(jnp.bfloat16)
        blocks = lax.all_to_all(near, FAR, 0, 0, tiled=True)
        return annual_tables(blocks, table, hits, years)

    last = sums.shape[1] // count
    branches = [functools.partial(exchanged, taken) for taken in range(1, last + 1)]
    twice = (strips[0] == last - 1) & (lax.axis_index("year") % 2 == 1)
    annual, kept, sent = lax.switch(
        jnp.where(twice, last, strips[0]), [*branches, exchanged_twice]
    )
    everyone = lax.all_to_all(sent, "year", 0, 0, tiled=True)
    net, stop_loss, tail_mean = outcomes(everyone, annual, kept, table)
    return (net.T, stop_loss.T, tail_mean.reshape(-1))


def solution(mesh):
    years, ports = mesh.shape["year"], mesh.shape["port"]
    port = (FAR, *NEAR)
    fine = Mesh(mesh.devices.reshape(years, ports // SQUARE, 2, 2), ("year", *port))
    return jax.shard_map(
        on_device,
        mesh=fine,
        in_specs=(
            P("year", port),
            P("year"),
            P(port),
            P(port),
            P(port, None),
            P(port, None),
            *([P(port)] * 6),
        ),
        out_specs=(P(port, "year"), P(port, "year"), P(port)),
        check_vma=False,
    )
```

```python
import functools

import jax
import jax.numpy as jnp
from jax import lax
from jax.experimental import pallas as pl
from jax.experimental.pallas import tpu as pltpu
from jax.sharding import PartitionSpec as P

TREATIES = 1024
MEMB = 4
YEAR_DEV = 32
TAIL = 16
LANES = 128
BLOCK = 256

UNIT_LOSS = 1.0

VMEM = pl.BlockSpec(memory_space=pltpu.VMEM)
SMEM = pl.BlockSpec(memory_space=pltpu.SMEM)
HBM = pl.BlockSpec(memory_space=pltpu.HBM)
PARAMS = pltpu.CompilerParams(vmem_limit_bytes=16 * 1024 * 1024)
BY_ROWS = (((1,), (1,)), ((), ()))


def clamp_between(values, lower, upper):
    return jnp.minimum(jnp.maximum(values, lower), upper)


def shard_sums_kernel(*refs):
    inputs, outputs, held = refs[:12], refs[12:16], refs[16:28]
    sums, table, hits, strips = outputs
    weights, ceded, arrived = refs[28:]
    count = table.shape[1]
    order = (5, 4, 0, 2, 3, 1, 6, 7, 8, 9, 10, 11)
    fetches = {
        k: pltpu.make_async_copy(inputs[k], held[k], arrived.at[k]) for k in order
    }
    for k in order:
        fetches[k].start()
    loss, year, retention, risk_limit, share, member = held[:6]
    columns = loss.shape[1]
    treaty = lax.broadcasted_iota(jnp.int32, (BLOCK, LANES), 0)
    treaty = treaty.astype(jnp.float32).astype(jnp.bfloat16)
    zero = jnp.zeros((BLOCK, LANES), jnp.bfloat16)
    fetches[5].wait()
    fetches[4].wait()
    named = member[...]
    part = share[...]

    def build(first):
        local = named - first
        inside = (local >= 0) & (local < BLOCK)
        local = jnp.where(inside, local, BLOCK).astype(jnp.float32).astype(jnp.bfloat16)
        for at in range(0, columns, LANES):
            block = zero
            for slot in range(MEMB):
                hit = treaty == local[slot : slot + 1, at : at + LANES]
                block = jnp.where(hit, part[slot : slot + 1, at : at + LANES], block)
            weights[first : first + BLOCK, at : at + LANES] = block

    def multiply(first):
        block = lax.dot_general(
            weights[first : first + BLOCK, :],
            ceded[...],
            BY_ROWS,
            preferred_element_type=jnp.float32,
        ).astype(jnp.bfloat16)
        for owner in range(BLOCK // count):
            for strip in range(block.shape[1] // LANES):
                sums[first // count + owner, strip * count : (strip + 1) * count, :] = block[
                    owner * count : (owner + 1) * count, strip * LANES : (strip + 1) * LANES
                ]

    blocks = list(range(0, TREATIES, BLOCK))
    ahead = 1
    for first in blocks[:ahead]:
        build(first)
    fetches[1].wait()
    local_year = jnp.where(year[...] < 0, -1, year[...] & (YEAR_DEV - 1))
    hit = lax.broadcasted_iota(jnp.int32, hits.shape, 0) == local_year
    hits[...] = jnp.where(hit, 1.0, 0.0).astype(jnp.bfloat16)
    strip = lax.broadcasted_iota(jnp.int32, year.shape, 1) // LANES
    strips[0] = jnp.max(jnp.where(year[...] >= 0, strip, 0))
    for row in range(6):
        fetches[6 + row].wait()
        table[row : row + 1, :] = held[6 + row][...].astype(jnp.float32)
    fetches[2].wait()
    fetches[3].wait()
    fetches[0].wait()
    ceded[...] = clamp_between(
        loss[...].astype(jnp.float32) - retention[...], 0.0, risk_limit[...]
    ).astype(jnp.bfloat16)
    for k, first in enumerate(blocks):
        multiply(first)
        if k + ahead < len(blocks):
            build(blocks[k + ahead])


def shard_sums(inputs):
    rows, columns = inputs[0].shape
    count = inputs[6].shape[0]
    views = [
        inputs[0],
        inputs[1].reshape(1, -1),
        inputs[2].reshape(1, -1),
        inputs[3].reshape(1, -1),
        inputs[4].T,
        inputs[5].T,
        *(column.reshape(1, -1) for column in inputs[6:]),
    ]
    views = [pltpu.with_memory_space_constraint(view, pltpu.HBM) for view in views]
    return pl.pallas_call(
        shard_sums_kernel,
        out_shape=(
            jax.ShapeDtypeStruct((TREATIES // count, rows // LANES * count, LANES), jnp.bfloat16),
            jax.ShapeDtypeStruct((8, count), jnp.float32),
            jax.ShapeDtypeStruct((YEAR_DEV, rows), jnp.bfloat16),
            pltpu.SMEM((1,), jnp.int32),
        ),
        in_specs=[HBM] * len(views),
        out_specs=(VMEM, VMEM, VMEM, SMEM),
        scratch_shapes=[
            *(pltpu.VMEM(view.shape, view.dtype) for view in views),
            pltpu.VMEM((TREATIES, columns), jnp.bfloat16),
            pltpu.VMEM((rows, columns), jnp.bfloat16),
            pltpu.SemaphoreType.DMA((len(views),)),
        ],
        compiler_params=PARAMS,
        name="shard_sums",
    )(*views)


def as_column(row):
    count = row.shape[1]
    down = lax.broadcasted_iota(jnp.int32, (count, count), 0)
    across = lax.broadcasted_iota(jnp.int32, (count, count), 1)
    return jnp.sum(jnp.where(down == across, row, 0.0), axis=1, keepdims=True)


def in_two(values):
    high = values.astype(jnp.bfloat16)
    low = (values - high.astype(jnp.float32)).astype(jnp.bfloat16)
    return [high, low]


def exchange(items, low, high):
    items[low], items[high] = (
        jnp.maximum(items[low], items[high]),
        jnp.minimum(items[low], items[high]),
    )


def sort_falling(items):
    count = len(items)
    step = 1
    while step < count:
        gap = step
        while gap >= 1:
            for base in range(gap % step, count - gap, 2 * gap):
                for at in range(base, base + min(gap, count - base - gap)):
                    if at // (2 * step) == (at + gap) // (2 * step):
                        exchange(items, at, at + gap)
            gap //= 2
        step *= 2


def larger_half(first, second):
    return [jnp.maximum(one, two) for one, two in zip(first, reversed(second))]


def sort_bitonic(items):
    gap = len(items) // 2
    while gap >= 1:
        for at in range(len(items)):
            if at & gap == 0:
                exchange(items, at, at + gap)
        gap //= 2


def annual_kernel(blocks, table, hits, annual, kept, sent):
    count = table.shape[1]
    parts = []
    for at in range(0, blocks.shape[1], count):
        part = blocks[0, at : at + count, :].astype(jnp.float32)
        for shard in range(1, blocks.shape[0]):
            part = part + blocks[shard, at : at + count, :].astype(jnp.float32)
        parts.append(part)
    total = jnp.concatenate(parts, axis=1)
    attach = table[0:1, :] * UNIT_LOSS
    limit = table[1:2, :] * UNIT_LOSS
    recovered = clamp_between(total - as_column(attach), 0.0, as_column(limit))
    retained = total - recovered
    pieces = jnp.concatenate(in_two(recovered) + in_two(retained), axis=0)
    yearly = lax.dot_general(
        hits[:, : total.shape[1]], pieces, BY_ROWS, preferred_element_type=jnp.float32
    )
    annual[...] = yearly[:, :count] + yearly[:, count : 2 * count]
    kept_annual = yearly[:, 2 * count : 3 * count] + yearly[:, 3 * count :]
    kept[...] = kept_annual
    line = jnp.concatenate((kept_annual[:TAIL], kept_annual[TAIL:]), axis=1)
    years = [jnp.broadcast_to(line[k : k + 1], (8, 2 * count)) for k in range(TAIL)]
    sort_falling(years)
    years = larger_half(years, [pltpu.roll(item, count, 1) for item in years])[: TAIL // 2]
    summed = jnp.sum(kept_annual, axis=0, keepdims=True)
    high, low = [part.astype(jnp.float32) for part in in_two(summed)]
    sums = jnp.broadcast_to(jnp.concatenate((high, low), axis=1), (8, 2 * count))
    rows = years + [sums] * 4
    down = lax.broadcasted_iota(jnp.int32, (8, 2 * count), 0)
    for chunk in range(3):
        packed = rows[4 * chunk + 3]
        for k in range(3):
            packed = jnp.where(down == k, rows[4 * chunk + k], packed)
        packed = packed[:4].astype(jnp.bfloat16)
        for peer in range(sent.shape[0]):
            sent[peer, :, 2 * count * chunk : 2 * count * (chunk + 1)] = packed


def annual_tables(blocks, table, hits, peers):
    count = table.shape[1]
    tables = jax.ShapeDtypeStruct((YEAR_DEV, count), jnp.float32)
    return pl.pallas_call(
        annual_kernel,
        out_shape=(
            tables,
            tables,
            jax.ShapeDtypeStruct((peers, 4, 6 * count), jnp.bfloat16),
        ),
        in_specs=[VMEM] * 3,
        out_specs=(VMEM, VMEM, VMEM),
        compiler_params=PARAMS,
        name="annual_tables",
    )(blocks, table, hits)


def outcome_kernel(everyone, annual, kept, table, net, stop_loss, tail_mean):
    limit = table[1:2, :] * UNIT_LOSS
    again = table[2:3, :]
    rate = table[3:4, :]
    paid = jnp.minimum(annual[...], (1.0 + again) * limit)
    net[...] = (paid - rate * jnp.minimum(paid, again * limit)) / limit
    peers = everyone.shape[0]
    count = everyone.shape[2] // 6
    lanes = 2 * count

    def chunk(peer, at, rows):
        return everyone[peer, :rows, at * lanes : (at + 1) * lanes].astype(jnp.float32)

    tiles = [
        jnp.concatenate((chunk(peer, at, 4), chunk(peer + 1, at, 4)), axis=0)
        for peer in range(0, peers, 2)
        for at in range(2)
    ]
    summed = chunk(0, 2, 4)
    for peer in range(1, peers):
        summed = summed + chunk(peer, 2, 4)
    summed = summed[:1]
    summed = summed + pltpu.roll(summed, count, 1)
    base_loss = UNIT_LOSS + summed / (peers * YEAR_DEV)
    largest = None
    for at in range(0, len(tiles), TAIL):
        group = tiles[at : at + TAIL]
        sort_falling(group)
        if largest is None:
            largest = group
        else:
            largest = larger_half(largest, group)
            sort_bitonic(largest)
    for shift in (4, 2, 1):
        largest = larger_half(largest, [pltpu.roll(item, shift, 0) for item in largest])
        sort_bitonic(largest)
    largest = larger_half(largest, [pltpu.roll(item, count, 1) for item in largest])
    top = largest[0]
    for item in largest[1:]:
        top = top + item
    tail_mean[...] = (top[0:1, :] / base_loss / TAIL)[:, :count]
    stop_loss[...] = clamp_between(
        kept[...] / base_loss[:, :count] - table[4:5, :], 0.0, table[5:6, :]
    )


def outcomes(everyone, annual, kept, table):
    return pl.pallas_call(
        outcome_kernel,
        out_shape=(
            jax.ShapeDtypeStruct(kept.shape, jnp.float32),
            jax.ShapeDtypeStruct(kept.shape, jnp.float32),
            jax.ShapeDtypeStruct((1, kept.shape[1]), jnp.float32),
        ),
        in_specs=[VMEM] * 4,
        out_specs=(VMEM, VMEM, VMEM),
        compiler_params=PARAMS,
        name="outcomes",
    )(everyone, annual, kept, table)


def on_device(*inputs):
    years = lax.axis_size("year")
    sums, table, hits, strips = shard_sums(inputs)
    count = table.shape[1]

    def exchanged(taken):
        rows = sums[:, : taken * count, :]
        blocks = lax.all_to_all(rows, "port", 0, 0, tiled=True)
        return annual_tables(blocks, table, hits, years)

    branches = [
        functools.partial(exchanged, taken + 1) for taken in range(sums.shape[1] // count)
    ]
    annual, kept, sent = lax.switch(strips[0], branches)
    everyone = lax.all_to_all(sent, "year", 0, 0, tiled=True)
    net, stop_loss, tail_mean = outcomes(everyone, annual, kept, table)
    return (net.T, stop_loss.T, tail_mean.reshape(-1))


def solution(mesh):
    return jax.shard_map(
        on_device,
        mesh=mesh,
        in_specs=(
            P("year", "port"),
            P("year"),
            P("port"),
            P("port"),
            P("port", None),
            P("port", None),
            P("port"),
            P("port"),
            P("port"),
            P("port"),
            P("port"),
            P("port"),
        ),
        out_specs=(P("port", "year"), P("port", "year"), P("port")),
        check_vma=False,
    )
```

```python
import functools

import jax
import jax.numpy as jnp
from jax import lax
from jax.experimental import pallas as pl
from jax.experimental.pallas import tpu as pltpu
from jax.sharding import PartitionSpec as P

TREATIES = 1024
MEMB = 4
YEAR_DEV = 32
TAIL = 16
LANES = 128
BLOCK = 256

UNIT_LOSS = 1.0

VMEM = pl.BlockSpec(memory_space=pltpu.VMEM)
SMEM = pl.BlockSpec(memory_space=pltpu.SMEM)
HBM = pl.BlockSpec(memory_space=pltpu.HBM)
PARAMS = pltpu.CompilerParams(vmem_limit_bytes=16 * 1024 * 1024)
BY_ROWS = (((1,), (1,)), ((), ()))


def clamp_between(values, lower, upper):
    return jnp.minimum(jnp.maximum(values, lower), upper)


def as_column(row):
    count = row.shape[1]
    down = lax.broadcasted_iota(jnp.int32, (count, count), 0)
    across = lax.broadcasted_iota(jnp.int32, (count, count), 1)
    return jnp.sum(jnp.where(down == across, row, 0.0), axis=1, keepdims=True)


def shard_sums_kernel(*refs):
    inputs, outputs, held = refs[:12], refs[12:17], refs[17:29]
    sums, table, columns_of, hits, strips = outputs
    weights, ceded, arrived = refs[29:]
    count = table.shape[1]
    order = (5, 4, 0, 2, 3, 1, 6, 7, 8, 9, 10, 11)
    fetches = {
        k: pltpu.make_async_copy(inputs[k], held[k], arrived.at[k]) for k in order
    }
    for k in order:
        fetches[k].start()
    loss, year, retention, risk_limit, share, member = held[:6]
    columns = loss.shape[1]
    treaty = lax.broadcasted_iota(jnp.int32, (BLOCK, LANES), 0)
    treaty = treaty.astype(jnp.float32).astype(jnp.bfloat16)
    zero = jnp.zeros((BLOCK, LANES), jnp.bfloat16)
    fetches[5].wait()
    fetches[4].wait()
    named = member[...]
    part = share[...]

    def build(first):
        local = named - first
        inside = (local >= 0) & (local < BLOCK)
        local = jnp.where(inside, local, BLOCK).astype(jnp.float32).astype(jnp.bfloat16)
        for at in range(0, columns, LANES):
            block = zero
            for slot in range(MEMB):
                hit = treaty == local[slot : slot + 1, at : at + LANES]
                block = jnp.where(hit, part[slot : slot + 1, at : at + LANES], block)
            weights[first : first + BLOCK, at : at + LANES] = block

    def multiply(first):
        block = lax.dot_general(
            weights[first : first + BLOCK, :],
            ceded[...],
            BY_ROWS,
            preferred_element_type=jnp.float32,
        ).astype(jnp.bfloat16)
        for owner in range(BLOCK // count):
            for strip in range(block.shape[1] // LANES):
                sums[first // count + owner, strip * count : (strip + 1) * count, :] = block[
                    owner * count : (owner + 1) * count, strip * LANES : (strip + 1) * LANES
                ]

    blocks = list(range(0, TREATIES, BLOCK))
    ahead = 1
    for first in blocks[:ahead]:
        build(first)
    fetches[1].wait()
    local_year = jnp.where(year[...] < 0, -1, year[...] & (YEAR_DEV - 1))
    hit = lax.broadcasted_iota(jnp.int32, hits.shape, 0) == local_year
    hits[...] = jnp.where(hit, 1.0, 0.0).astype(jnp.bfloat16)
    strip = lax.broadcasted_iota(jnp.int32, year.shape, 1) // LANES
    strips[0] = jnp.max(jnp.where(year[...] >= 0, strip, 0))
    for row in range(6):
        fetches[6 + row].wait()
        table[row : row + 1, :] = held[6 + row][...].astype(jnp.float32)
    for row in range(2):
        column = as_column(table[row : row + 1, :] * UNIT_LOSS)
        columns_of[row] = jnp.broadcast_to(column, columns_of.shape[1:])
    fetches[2].wait()
    fetches[3].wait()
    fetches[0].wait()
    ceded[...] = clamp_between(
        loss[...].astype(jnp.float32) - retention[...], 0.0, risk_limit[...]
    ).astype(jnp.bfloat16)
    for k, first in enumerate(blocks):
        multiply(first)
        if k + ahead < len(blocks):
            build(blocks[k + ahead])


def shard_sums(inputs):
    rows, columns = inputs[0].shape
    count = inputs[6].shape[0]
    views = [
        inputs[0],
        inputs[1].reshape(1, -1),
        inputs[2].reshape(1, -1),
        inputs[3].reshape(1, -1),
        inputs[4].T,
        inputs[5].T,
        *(column.reshape(1, -1) for column in inputs[6:]),
    ]
    views = [pltpu.with_memory_space_constraint(view, pltpu.HBM) for view in views]
    return pl.pallas_call(
        shard_sums_kernel,
        out_shape=(
            jax.ShapeDtypeStruct((TREATIES // count, rows // LANES * count, LANES), jnp.bfloat16),
            jax.ShapeDtypeStruct((8, count), jnp.float32),
            jax.ShapeDtypeStruct((2, count, LANES), jnp.float32),
            jax.ShapeDtypeStruct((YEAR_DEV, rows), jnp.bfloat16),
            pltpu.SMEM((1,), jnp.int32),
        ),
        in_specs=[HBM] * len(views),
        out_specs=(VMEM, VMEM, VMEM, VMEM, SMEM),
        scratch_shapes=[
            *(pltpu.VMEM(view.shape, view.dtype) for view in views),
            pltpu.VMEM((TREATIES, columns), jnp.bfloat16),
            pltpu.VMEM((rows, columns), jnp.bfloat16),
            pltpu.SemaphoreType.DMA((len(views),)),
        ],
        compiler_params=PARAMS,
        name="shard_sums",
    )(*views)


def in_two(values):
    high = values.astype(jnp.bfloat16)
    low = (values - high.astype(jnp.float32)).astype(jnp.bfloat16)
    return [high, low]


def exchange(items, low, high):
    items[low], items[high] = (
        jnp.maximum(items[low], items[high]),
        jnp.minimum(items[low], items[high]),
    )


def sort_falling(items):
    count = len(items)
    step = 1
    while step < count:
        gap = step
        while gap >= 1:
            for base in range(gap % step, count - gap, 2 * gap):
                for at in range(base, base + min(gap, count - base - gap)):
                    if at // (2 * step) == (at + gap) // (2 * step):
                        exchange(items, at, at + gap)
            gap //= 2
        step *= 2


def larger_half(first, second):
    return [jnp.maximum(one, two) for one, two in zip(first, reversed(second))]


def sort_bitonic(items):
    gap = len(items) // 2
    while gap >= 1:
        for at in range(len(items)):
            if at & gap == 0:
                exchange(items, at, at + gap)
        gap //= 2


def annual_kernel(blocks, columns_of, hits, annual, kept, sent):
    count = columns_of.shape[1]
    attach, limit = columns_of[0], columns_of[1]
    recovered, retained = [], []
    for at in range(0, blocks.shape[1], count):
        total = blocks[0, at : at + count, :].astype(jnp.float32)
        for shard in range(1, blocks.shape[0]):
            total = total + blocks[shard, at : at + count, :].astype(jnp.float32)
        recovered.append(clamp_between(total - attach, 0.0, limit))
        retained.append(total - recovered[-1])
    pieces = [
        jnp.concatenate(strips, axis=1)
        for strips in (*zip(*map(in_two, recovered)), *zip(*map(in_two, retained)))
    ]
    pieces = jnp.concatenate(pieces, axis=0)
    yearly = lax.dot_general(
        hits[:, : pieces.shape[1]], pieces, BY_ROWS, preferred_element_type=jnp.float32
    )
    annual[...] = yearly[:, :count] + yearly[:, count : 2 * count]
    kept_annual = yearly[:, 2 * count : 3 * count] + yearly[:, 3 * count :]
    kept[...] = kept_annual
    line = jnp.concatenate((kept_annual[:TAIL], kept_annual[TAIL:]), axis=1)
    years = [jnp.broadcast_to(line[k : k + 1], (8, 2 * count)) for k in range(TAIL)]
    sort_falling(years)
    years = larger_half(years, [pltpu.roll(item, count, 1) for item in years])[: TAIL // 2]
    summed = jnp.sum(kept_annual, axis=0, keepdims=True)
    high, low = [part.astype(jnp.float32) for part in in_two(summed)]
    sums = jnp.broadcast_to(jnp.concatenate((high, low), axis=1), (8, 2 * count))
    rows = years + [sums] * 4
    down = lax.broadcasted_iota(jnp.int32, (8, 2 * count), 0)
    for chunk in range(3):
        packed = rows[4 * chunk + 3]
        for k in range(3):
            packed = jnp.where(down == k, rows[4 * chunk + k], packed)
        packed = packed[:4].astype(jnp.bfloat16)
        for peer in range(sent.shape[0]):
            sent[peer, :, 2 * count * chunk : 2 * count * (chunk + 1)] = packed


def annual_tables(blocks, columns_of, hits, peers):
    count = columns_of.shape[1]
    tables = jax.ShapeDtypeStruct((YEAR_DEV, count), jnp.float32)
    return pl.pallas_call(
        annual_kernel,
        out_shape=(
            tables,
            tables,
            jax.ShapeDtypeStruct((peers, 4, 6 * count), jnp.bfloat16),
        ),
        in_specs=[VMEM] * 3,
        out_specs=(VMEM, VMEM, VMEM),
        compiler_params=PARAMS,
        name="annual_tables",
    )(blocks, columns_of, hits)


def outcome_kernel(everyone, annual, kept, table, net, stop_loss, tail_mean):
    limit = table[1:2, :] * UNIT_LOSS
    again = table[2:3, :]
    rate = table[3:4, :]
    paid = jnp.minimum(annual[...], (1.0 + again) * limit)
    net[...] = (paid - rate * jnp.minimum(paid, again * limit)) / limit
    peers = everyone.shape[0]
    count = everyone.shape[2] // 6
    lanes = 2 * count

    def chunk(peer, at, rows):
        return everyone[peer, :rows, at * lanes : (at + 1) * lanes].astype(jnp.float32)

    tiles = [
        jnp.concatenate((chunk(peer, at, 4), chunk(peer + 1, at, 4)), axis=0)
        for peer in range(0, peers, 2)
        for at in range(2)
    ]
    summed = chunk(0, 2, 4)
    for peer in range(1, peers):
        summed = summed + chunk(peer, 2, 4)
    summed = summed[:1]
    summed = summed + pltpu.roll(summed, count, 1)
    base_loss = UNIT_LOSS + summed / (peers * YEAR_DEV)
    largest = None
    for at in range(0, len(tiles), TAIL):
        group = tiles[at : at + TAIL]
        sort_falling(group)
        if largest is None:
            largest = group
        else:
            largest = larger_half(largest, group)
            sort_bitonic(largest)
    for shift in (4, 2, 1):
        largest = larger_half(largest, [pltpu.roll(item, shift, 0) for item in largest])
        sort_bitonic(largest)
    largest = larger_half(largest, [pltpu.roll(item, count, 1) for item in largest])
    top = largest[0]
    for item in largest[1:]:
        top = top + item
    tail_mean[...] = (top[0:1, :] / base_loss / TAIL)[:, :count]
    stop_loss[...] = clamp_between(
        kept[...] / base_loss[:, :count] - table[4:5, :], 0.0, table[5:6, :]
    )


def outcomes(everyone, annual, kept, table):
    return pl.pallas_call(
        outcome_kernel,
        out_shape=(
            jax.ShapeDtypeStruct(kept.shape, jnp.float32),
            jax.ShapeDtypeStruct(kept.shape, jnp.float32),
            jax.ShapeDtypeStruct((1, kept.shape[1]), jnp.float32),
        ),
        in_specs=[VMEM] * 4,
        out_specs=(VMEM, VMEM, VMEM),
        compiler_params=PARAMS,
        name="outcomes",
    )(everyone, annual, kept, table)


def on_device(*inputs):
    years = lax.axis_size("year")
    sums, table, columns_of, hits, strips = shard_sums(inputs)
    count = table.shape[1]

    def exchanged(taken):
        rows = sums[:, : taken * count, :]
        blocks = lax.all_to_all(rows, "port", 0, 0, tiled=True)
        return annual_tables(blocks, columns_of, hits, years)

    branches = [
        functools.partial(exchanged, taken + 1) for taken in range(sums.shape[1] // count)
    ]
    annual, kept, sent = lax.switch(strips[0], branches)
    everyone = lax.all_to_all(sent, "year", 0, 0, tiled=True)
    net, stop_loss, tail_mean = outcomes(everyone, annual, kept, table)
    return (net.T, stop_loss.T, tail_mean.reshape(-1))


def solution(mesh):
    return jax.shard_map(
        on_device,
        mesh=mesh,
        in_specs=(
            P("year", "port"),
            P("year"),
            P("port"),
            P("port"),
            P("port", None),
            P("port", None),
            P("port"),
            P("port"),
            P("port"),
            P("port"),
            P("port"),
            P("port"),
        ),
        out_specs=(P("port", "year"), P("port", "year"), P("port")),
        check_vma=False,
    )
```
